256 devices in a mesh: shot: 32 (over y, z), depth: 8 (over x, core).
Axes of the slice: x: 4, y: 4, z: 8, core: 2. Of those that a mesh axis runs over, the one named last changes fastest.
Arguments:
- correlation: float32 [64, 64, 32, 1024], P('shot', None, None, 'depth'), may hold values from -6 to 6
- illumination: float32 [64, 64, 32, 1024], P('shot', None, None, 'depth'), may hold values from 0.25 to 4
- aperture: int32 [64, 4], P('shot'), may hold values from 0 to 64, as said below
Outputs:
- stack: float32 [64, 32, 1024], P('shot', None, 'depth')
The draws below stay inside these ranges and needn't reach their ends.
Inputs may be any that keep to these rules, and one draw needn't show every extreme that they name: For every shot, 0 <= aperture[s,0] < aperture[s,1] <= 64 and 0 <= aperture[s,2] < aperture[s,3] <= 32; each box spans a quarter to a half of the grid along each of the two dimensions.
All inputs are finite; a program needn't handle non-finite values.
Results may differ from the reference program's by a relative error of at most 0.0003.
Values sent between devices are 32-bit elements.
A program may use at most 64 MiB of HBM per device.

```python
import math
import jax
import jax.numpy as jnp
from jax import lax

NY = 32
SHOTS = 64
NX = 64
NZ = 1024


def draw_aperture(key, part):
    key_first = jax.random.fold_in(key, 11)
    key_second = jax.random.fold_in(key, 23)
    k_one, k_two = jax.random.split(key_first)
    k_three, k_four = jax.random.split(key_second)
    low_first = jax.random.randint(k_one, (SHOTS,), 0, NX // 2)
    span_first = jax.random.randint(k_two, (SHOTS,), max(NX // 4, 1), NX // 2 + 1)
    low_second = jax.random.randint(k_three, (SHOTS,), 0, NY // 2)
    span_second = jax.random.randint(k_four, (SHOTS,), max(NY // 4, 1), NY // 2 + 1)
    return jnp.stack([low_first, low_first + span_first, low_second, low_second + span_second], axis=1).astype(jnp.int32)


def spiked(values, rng, source, target, blocks, factor):
    owner, partner = [(jnp.arange(values.shape[position]) // (values.shape[position] // blocks)).reshape([-1 if axis == position else 1 for axis in range(values.ndim)]) for position in (source, target)]
    chosen = jax.random.permutation(rng, blocks)[partner]
    strong = (owner == chosen) | (owner == (partner + blocks // 2) % blocks)
    return jnp.where(strong, factor * values, values)


def steps_of(stream_key, dims, pieces, smallest, high):
    def one(dim, blocks):
        draws = jax.random.uniform(jax.random.fold_in(jax.random.fold_in(stream_key, 6), dim), (blocks,), jnp.float32, smallest / len(pieces), high / len(pieces))
        return jnp.repeat(jnp.exp(draws), dims[dim] // blocks).reshape((-1,) + (1,) * (len(dims) - dim - 1))

    gain = one(*pieces[0])
    for cut in pieces[1:]:
        gain = gain * one(*cut)
    return gain


def gaussian_with(stream_key, dims, width, most, pieces, heavy, kind=jnp.bfloat16):
    array = width * jax.random.normal(stream_key, dims, jnp.float32)
    if pieces:
        array = array * steps_of(stream_key, dims, pieces, -0.22, 0.18)
    return jnp.clip(spiked(array, jax.random.fold_in(stream_key, 3), *heavy), -most, most).astype(kind)


def setup_inputs(seed: int = 0) -> dict:
    seeds = jax.random.split(jax.random.key(seed), 4)
    correlation = gaussian_with(seeds[0], (SHOTS, NX, NY, NZ), 1.0, 6.0, ((0, 32), (3, 8)), (0, 1, 32, 2.75), jnp.float32)
    illumination = jnp.clip(jnp.exp(math.log(4.0) - 2.7725887 * jax.random.uniform(seeds[1], (SHOTS, NX, NY, NZ), jnp.float32) ** steps_of(seeds[1], (SHOTS, NX, NY, NZ), ((0, 32), (3, 8)), -0.2, 0.2)), 0.25, 4.0)
    aperture = draw_aperture(jax.random.fold_in(seeds[3], 71), 0)
    return {"correlation": correlation, "illumination": illumination, "aperture": aperture}


def negative_laplacian(field):
    padded = jnp.pad(field, 1)
    beside = padded[2:, 1:-1, 1:-1] + padded[:-2, 1:-1, 1:-1]
    beside = beside + padded[1:-1, 2:, 1:-1] + padded[1:-1, :-2, 1:-1]
    beside = beside + padded[1:-1, 1:-1, 2:] + padded[1:-1, 1:-1, :-2]
    return 6.0 * field - beside

def prepare(correlation, illumination, box):
    first = lax.broadcasted_iota(jnp.int32, (NX, NY, 1), 0)
    second = lax.broadcasted_iota(jnp.int32, (NX, NY, 1), 1)
    inside = (first >= box[0]) & (first < box[1]) & (second >= box[2]) & (second < box[3])
    mask = inside.astype(jnp.float32)
    return negative_laplacian(mask * correlation / (illumination + 0.1))

def reference(correlation, illumination, aperture):
    cells = NX * NY * NZ

    def energy(items):
        filtered = prepare(items[0], items[1], items[2])
        return jnp.sum(filtered * filtered) / cells
    meansq = lax.map(energy, (correlation, illumination, aperture))
    peak = jnp.max(meansq)
    weight = 1.0 / jnp.sqrt(meansq + 0.5 * peak + 1.0)

    def accumulate(total, items):
        filtered = prepare(items[0], items[1], items[2])
        return (total + items[3] * filtered, None)
    stack, unused = lax.scan(accumulate, jnp.zeros((NX, NY, NZ), jnp.float32), (correlation, illumination, aperture, weight))
    return stack / jnp.sqrt(jnp.float32(SHOTS))
```

```python
import functools

import jax
import jax.numpy as jnp
from jax import lax
from jax.experimental import pallas as pl
from jax.experimental.pallas import tpu as pltpu
from jax.sharding import PartitionSpec as P

ROWS_Y = 4
PIECES = 4
F32 = jnp.float32


def kernel(
    ny_dev, nz_dev, nd_dev,
    box, corr, illum, out,
    corr_v, illum_v, filt, edge, edge_low, edge_high, energy, peaks,
    raw_up, raw_down, weighted, got_up, got_down, image, arrived,
    load_sem, edge_send, edge_recv, small_send, small_recv,
    raw_send, raw_recv, move_send, move_recv, last_send, last_recv,
):
    shots, nx, ny, nz = filt.shape
    shot, depth = lax.axis_index("shot"), lax.axis_index("depth")
    y, z = shot // nz_dev, shot % nz_dev
    per_y = nx // ny_dev
    per_z = per_y // nz_dev
    half = per_y // 2

    step = nx // PIECES
    loads = []
    for s in range(shots):
        for c in range(PIECES):
            rows = pl.ds(c * step, step)
            pair = [
                pltpu.make_async_copy(corr.at[s, rows], corr_v.at[s, rows], load_sem.at[s, c, 0]),
                pltpu.make_async_copy(illum.at[s, rows], illum_v.at[s, rows], load_sem.at[s, c, 1]),
            ]
            for copy in pair:
                copy.start()
            loads.append(pair)

    near = []
    for dy in range(ny_dev):
        for dd in range(nd_dev):
            if dy or dd:
                near.append({
                    "shot": lax.rem(y + dy, ny_dev) * nz_dev + z,
                    "depth": lax.rem(depth + dd, nd_dev),
                })
    along = [
        {"shot": y * nz_dev + lax.rem(z + dz, nz_dev), "depth": depth} for dz in range(1, nz_dev)
    ]
    barrier = pltpu.get_barrier_semaphore()
    for peer in near + along:
        pl.semaphore_signal(barrier, inc=1, device_id=peer, device_id_type=pl.DeviceIdType.MESH)

    lane = lax.broadcasted_iota(jnp.int32, (ny, nz), 1)
    row = lax.broadcasted_iota(jnp.int32, (ny, nz), 0)
    first, last = lane == 0, lane == nz - 1
    top, bottom = row == 0, row == ny - 1
    column = lane // 2
    zero = jnp.zeros((ny, nz), F32)

    sums, packs = [], []
    for s in range(shots):
        low, high = box[s, 0], box[s, 1]
        strip = ((row >= box[s, 2]) & (row < box[s, 3])).astype(F32)

        def normal(x, s=s, low=low, high=high, strip=strip):
            inside = jnp.where((x >= low) & (x < high), 1.0, 0.0).astype(F32)
            return (strip * inside) * corr_v[s, x] / (illum_v[s, x] + 0.1)

        def filtered(before, here, after):
            beside = before + after
            beside = beside + jnp.where(top, 0.0, pltpu.roll(here, 1, 0))
            beside = beside + jnp.where(bottom, 0.0, pltpu.roll(here, ny - 1, 0))
            beside = beside + jnp.where(first, 0.0, pltpu.roll(here, 1, 1))
            beside = beside + jnp.where(last, 0.0, pltpu.roll(here, nz - 1, 1))
            return 6.0 * here - beside

        def one(x, after, carry, s=s):
            before, here, mine, rim, total = carry
            value = filtered(before, here, after)
            filt[s, x] = value
            chosen = column == x
            mine = jnp.where(chosen, pltpu.roll(here, lax.rem(2 * x + 1, nz), 1), mine)
            rim = jnp.where(chosen, pltpu.roll(value, lax.rem(2 * x + 1, nz), 1), rim)
            total = total + jnp.where(first | last, 0.0, value * value)
            return here, after, mine, rim, total

        for copy in loads[s * PIECES]:
            copy.wait()
        carry = (zero, normal(0), zero, zero, zero)
        for c in range(PIECES):
            if c:
                for copy in loads[s * PIECES + c]:
                    copy.wait()
            carry = lax.fori_loop(
                c * step + (c == 0), (c + 1) * step,
                lambda x, carry: one(x - 1, normal(x), carry), carry,
            )
        carry = one(nx - 1, zero, carry)
        edge[s] = carry[2]
        packs.append(carry[3])
        sums.append(carry[4])

    pl.semaphore_wait(barrier, len(near) + len(along))

    def remote(src, dst, send, recv, peer):
        return pltpu.make_async_remote_copy(
            src_ref=src, dst_ref=dst, send_sem=send, recv_sem=recv,
            device_id=peer, device_id_type=pl.DeviceIdType.MESH,
        )

    up = remote(edge, edge_low, edge_send.at[0], edge_recv.at[0], {"shot": shot, "depth": lax.rem(depth + 1, nd_dev)})
    down = remote(edge, edge_high, edge_send.at[1], edge_recv.at[1], {"shot": shot, "depth": lax.rem(depth + nd_dev - 1, nd_dev)})

    @pl.when(depth < nd_dev - 1)
    def _():
        up.start()

    @pl.when(depth > 0)
    def _():
        down.start()

    @pl.when(depth == 0)
    def _():
        edge_low[...] = jnp.zeros_like(edge_low)

    @pl.when(depth == nd_dev - 1)
    def _():
        edge_high[...] = jnp.zeros_like(edge_high)

    @pl.when(depth > 0)
    def _():
        up.wait_recv()

    @pl.when(depth < nd_dev - 1)
    def _():
        down.wait_recv()

    even = lax.rem(lane, 2) == 0
    sides = []
    for s in range(shots):
        side = jnp.where(even, pltpu.roll(edge_high[s], nz - 1, 1), pltpu.roll(edge_low[s], 1, 1))
        sides.append(side)
        rim = packs[s] - side
        energy[0, s : s + 1] = jnp.sum(sums[s] + rim * rim, axis=0, keepdims=True)

    spread = []
    for i, peer in enumerate(near):
        dy, dd = (i + 1) // nd_dev, (i + 1) % nd_dev
        slot = ((ny_dev - dy) % ny_dev) * nd_dev + (nd_dev - dd) % nd_dev
        copy = remote(energy.at[0], energy.at[slot], small_send.at[0], small_recv.at[0], peer)
        copy.start()
        spread.append(copy)

    ends = first | last

    def finish(base, count):
        def body(i, carry):
            x = base + i
            for s in range(shots):
                filt[s, x] = filt[s, x] - jnp.where(ends, pltpu.roll(sides[s], lax.rem(nz + nz - 1 - 2 * x, nz), 1), 0.0)
            return carry
        lax.fori_loop(0, count, body, 0)

    after = lax.rem(y + 1, ny_dev)
    before = lax.rem(y + ny_dev - 1, ny_dev)
    across = lax.rem(y + ny_dev // 2, ny_dev)
    next_y = {"shot": after * nz_dev + z, "depth": depth}
    prev_y = {"shot": before * nz_dev + z, "depth": depth}
    finish(across * per_y, half)
    raw_a = remote(filt.at[:, pl.ds(across * per_y, half)], raw_up, raw_send.at[0], raw_recv.at[0], next_y)
    raw_a.start()
    finish(across * per_y + half, half)
    raw_b = remote(filt.at[:, pl.ds(across * per_y + half, half)], raw_down, raw_send.at[1], raw_recv.at[1], prev_y)
    raw_b.start()
    finish(after * per_y, per_y)
    finish(before * per_y, per_y)
    finish(y * per_y, per_y)

    others = energy.at[pl.ds(1, len(near))]
    pltpu.make_async_copy(others, others, small_recv.at[0]).wait()
    cells = nx * ny * nz * nd_dev
    means = []
    for dy in range(ny_dev):
        both = jnp.sum(energy[dy * nd_dev : (dy + 1) * nd_dev], axis=0)
        means.append(jnp.broadcast_to(jnp.sum(both, axis=1, keepdims=True) / cells, (shots, nz)))
    peak = functools.reduce(jnp.maximum, means)
    peaks[0] = peak
    for i, peer in enumerate(along):
        slot = nz_dev - 1 - i
        copy = remote(peaks.at[0], peaks.at[slot], small_send.at[1], small_recv.at[1], peer)
        copy.start()
    rest = peaks.at[pl.ds(1, len(along))]
    pltpu.make_async_copy(rest, rest, small_recv.at[1]).wait()
    peak = jnp.max(jnp.max(peaks[...], axis=0), axis=0, keepdims=True)
    scale = 1.0 / float(shots * ny_dev * nz_dev) ** 0.5
    weights = [scale / jnp.sqrt(mean + 0.5 * peak + 1.0) for mean in means]

    def weight(dy, s):
        return jnp.broadcast_to(weights[dy][s : s + 1], (ny, nz))

    def own(base, count, extra=None):
        mine = [weight(0, s) for s in range(shots)]

        def body(i, carry):
            x = base + i
            value = sum(mine[s] * filt[s, x] for s in range(shots))
            if extra is not None:
                ref, dy = extra
                value = value + sum(weight(dy, s) * ref[s, i] for s in range(shots))
            weighted[x] = value
            return carry
        lax.fori_loop(0, count, body, 0)

    def move(base, dst, sem, peer):
        copy = remote(weighted.at[pl.ds(base, half)], dst, move_send.at[sem], move_recv.at[sem], peer)
        copy.start()
        return copy

    moves = []
    own(after * per_y + half, half)
    moves.append(move(after * per_y + half, got_up.at[pl.ds(half, half)], 0, next_y))
    own(before * per_y, half)
    moves.append(move(before * per_y, got_down.at[pl.ds(0, half)], 1, prev_y))
    raw_a.wait_recv()
    own(after * per_y, half, (raw_up, ny_dev - 1))
    moves.append(move(after * per_y, got_up.at[pl.ds(0, half)], 2, next_y))
    raw_b.wait_recv()
    own(before * per_y + half, half, (raw_down, 1))
    moves.append(move(before * per_y + half, got_down.at[pl.ds(half, half)], 3, prev_y))
    own(y * per_y, per_y)

    for copy in moves:
        copy.wait_recv()

    def merge(i, carry):
        image[i] = weighted[y * per_y + i] + got_up[i] + got_down[i]
        return carry
    lax.fori_loop(0, per_y, merge, 0)

    finals = {}
    for dz in sorted(range(1, nz_dev), key=lambda d: -min(d, nz_dev - d)):
        target = lax.rem(z + dz, nz_dev)
        slot = nz_dev - dz - 1
        copy = remote(
            image.at[pl.ds(target * per_z, per_z)], arrived.at[slot],
            last_send.at[dz - 1], last_recv.at[slot], along[dz - 1],
        )
        copy.start()
        finals[dz] = copy
    result = image[pl.ds(z * per_z, per_z)]
    for dz, copy in finals.items():
        copy.wait_recv()
        result = result + arrived[nz_dev - dz - 1]
    out[...] = result

    for copy in finals.values():
        copy.wait_send()
    for copy in moves + [raw_a, raw_b]:
        copy.wait_send()
    pltpu.make_async_copy(others, others, small_send.at[0]).wait()
    pltpu.make_async_copy(rest, rest, small_send.at[1]).wait()

    @pl.when(depth < nd_dev - 1)
    def _():
        up.wait_send()

    @pl.when(depth > 0)
    def _():
        down.wait_send()


def solution(mesh):
    nd_dev = mesh.shape["depth"]
    ny_dev = ROWS_Y
    nz_dev = mesh.shape["shot"] // ny_dev

    def on_device(correlation, illumination, aperture):
        shots, nx, ny, nz = correlation.shape
        per_y = nx // ny_dev
        per_z = per_y // nz_dev
        half = per_y // 2
        dma = pltpu.SemaphoreType.DMA
        return pl.pallas_call(
            functools.partial(kernel, ny_dev, nz_dev, nd_dev),
            out_shape=jax.ShapeDtypeStruct((per_z, ny, nz), F32),
            in_specs=[
                pl.BlockSpec(memory_space=pltpu.SMEM),
                pl.BlockSpec(memory_space=pl.ANY),
                pl.BlockSpec(memory_space=pl.ANY),
            ],
            out_specs=pl.BlockSpec(memory_space=pltpu.VMEM),
            scratch_shapes=[
                pltpu.VMEM((shots, nx, ny, nz), F32),
                pltpu.VMEM((shots, nx, ny, nz), F32),
                pltpu.VMEM((shots, nx, ny, nz), F32),
                pltpu.VMEM((shots, ny, nz), F32),
                pltpu.VMEM((shots, ny, nz), F32),
                pltpu.VMEM((shots, ny, nz), F32),
                pltpu.VMEM((ny_dev * nd_dev, shots, nz), F32),
                pltpu.VMEM((nz_dev, shots, nz), F32),
                pltpu.VMEM((shots, half, ny, nz), F32),
                pltpu.VMEM((shots, half, ny, nz), F32),
                pltpu.VMEM((nx, ny, nz), F32),
                pltpu.VMEM((per_y, ny, nz), F32),
                pltpu.VMEM((per_y, ny, nz), F32),
                pltpu.VMEM((per_y, ny, nz), F32),
                pltpu.VMEM((nz_dev - 1, per_z, ny, nz), F32),
                dma((shots, PIECES, 2)),
                dma((2,)), dma((2,)), dma((2,)), dma((2,)),
                dma((2,)), dma((2,)), dma((4,)), dma((4,)),
                dma((nz_dev - 1,)), dma((nz_dev - 1,)),
            ],
            compiler_params=pltpu.CompilerParams(
                collective_id=0, has_side_effects=True, vmem_limit_bytes=67_043_328
            ),
        )(aperture, correlation, illumination)

    return jax.shard_map(
        on_device,
        mesh=mesh,
        in_specs=(P("shot", None, None, "depth"), P("shot", None, None, "depth"), P("shot", None)),
        out_specs=P("shot", None, "depth"),
        check_vma=False,
    )
```

```python
import functools

import jax
import jax.numpy as jnp
from jax import lax
from jax.experimental import pallas as pl
from jax.experimental.pallas import tpu as pltpu
from jax.sharding import PartitionSpec as P

ROWS_Y = 4
PIECES = 4
UNROLL = 4
F32 = jnp.float32
MESH = pl.DeviceIdType.MESH


class Marks:
    def __init__(self):
        self.scope = None

    def __call__(self, name):
        if self.scope is not None:
            self.scope.__exit__(None, None, None)
            self.scope = None
        if name:
            self.scope = jax.named_scope(name)
            self.scope.__enter__()


def ring_order(count):
    return sorted(range(count), key=lambda d: (-min(d, count - d), d))


def kernel(
    ny_dev, nz_dev, nd_dev,
    box_hbm, corr, illum, out,
    box, corr_v, illum_v, norm, filt, edge, edge_low, edge_high, rim_v, side_v, mixed,
    energy, peaks, raw_out, raw_in, sent, got, image, arrived,
    box_sem, load_sem, edge_send, edge_recv, small_send, small_recv,
    raw_send, raw_recv, move_send, move_recv, last_send, last_recv,
):
    shots, nx, ny, nz = filt.shape
    mark = Marks()
    mark("p00_load_signal")
    shot, depth = lax.axis_index("shot"), lax.axis_index("depth")
    y, z = shot // nz_dev, shot % nz_dev
    per_y = nx // ny_dev
    group = nz // 4
    groups = nx // group

    box_load = pltpu.make_async_copy(box_hbm, box, box_sem)
    box_load.start()
    step = nx // PIECES
    loads = []
    for c in range(PIECES):
        piece = []
        for s in range(shots):
            rows = pl.ds(c * step, step)
            piece.append(pltpu.make_async_copy(corr.at[s, rows], corr_v.at[s, rows], load_sem.at[s, c, 0]))
            piece.append(pltpu.make_async_copy(illum.at[s, rows], illum_v.at[s, rows], load_sem.at[s, c, 1]))
        for copy in piece:
            copy.start()
        loads.append(piece)

    near = []
    for dy in range(ny_dev):
        for dd in range(nd_dev):
            if dy or dd:
                near.append({
                    "shot": lax.rem(y + dy, ny_dev) * nz_dev + z,
                    "depth": lax.rem(depth + dd, nd_dev),
                })
    along = [
        {"shot": y * nz_dev + lax.rem(z + dz, nz_dev), "depth": depth} for dz in range(1, nz_dev)
    ]
    barrier = pltpu.get_barrier_semaphore()
    for peer in near + along:
        pl.semaphore_signal(barrier, inc=1, device_id=peer, device_id_type=MESH)

    lane = lax.broadcasted_iota(jnp.int32, (ny, nz), 1)
    row = lax.broadcasted_iota(jnp.int32, (ny, nz), 0)
    first, last = lane == 0, lane == nz - 1
    ends = first | last
    top, bottom = row == 0, row == ny - 1
    column = lane // 4
    place = lax.rem(lane, 4)
    zero = jnp.zeros((ny, nz), F32)

    def beside_rows(here):
        return jnp.where(top, 0.0, pltpu.roll(here, 1, 0)) + jnp.where(bottom, 0.0, pltpu.roll(here, ny - 1, 0))

    box_load.wait()
    mark("p01_filter")
    strips = [((row >= box[s, 2]) & (row < box[s, 3])).astype(F32) for s in range(shots)]
    bounds = [(box[s, 0], box[s, 1]) for s in range(shots)]
    for s in range(shots):
        norm[s, 0] = zero
        norm[s, nx + 1] = zero

    def normalize(k, packs):
        packs = list(packs)
        for s in range(shots):
            for j in range(UNROLL):
                x = k * UNROLL + j
                inside = jnp.where((x >= bounds[s][0]) & (x < bounds[s][1]), 1.0, 0.0).astype(F32)
                value = (strips[s] * inside) * corr_v[s, x] / (illum_v[s, x] + 0.1)
                norm[s, x + 1] = value
                turned = pltpu.roll(value, lax.rem(4 * x + 2, nz), 1)
                packs[s] = jnp.where(column == lax.rem(x, group), turned, packs[s])
        return tuple(packs)

    def filter_block(k, sums):
        sums = list(sums)
        for s in range(shots):
            rows = [norm[s, k * UNROLL + i] for i in range(UNROLL + 2)]
            for j in range(UNROLL):
                here = rows[j + 1]
                beside = rows[j] + rows[j + 2] + beside_rows(here)
                beside = beside + jnp.where(first, 0.0, pltpu.roll(here, 1, 1))
                beside = beside + jnp.where(last, 0.0, pltpu.roll(here, nz - 1, 1))
                value = 6.0 * here - beside
                filt[s, k * UNROLL + j] = value
                sums[s] = sums[s] + value * value
        return tuple(sums)

    blocks = nx // UNROLL
    per_piece = step // UNROLL
    packs, sums, packed = (zero,) * shots, (zero,) * shots, []
    for c in range(PIECES):
        for copy in loads[c]:
            copy.wait()
        begin = c * per_piece
        if c == 0:
            for k in range(2):
                packs = normalize(k, packs)
            begin = 2

        def body(k, carry):
            packs, sums = carry
            sums = filter_block(k - 2, sums)
            return normalize(k, packs), sums

        packs, sums = lax.fori_loop(begin, (c + 1) * per_piece, body, (packs, sums))
        if (c + 1) * step % group == 0:
            packed.append(packs)
            packs = (zero,) * shots
    for k in (blocks - 2, blocks - 1):
        sums = filter_block(k, sums)

    mark("p02_pack")
    inner = (place == 1) | (place == 2)
    for s in range(shots):
        parts = [packed[g][s] for g in range(groups)]
        edge[s] = jnp.where(inner, parts[0], pltpu.roll(parts[1], 2, 1))
        backs = [pltpu.roll(part, 4, 1) for part in parts]
        aheads = [pltpu.roll(part, nz - 4, 1) for part in parts]
        for g, part in enumerate(parts):
            back = jnp.where(lane < 4, backs[g - 1] if g else 0.0, backs[g])
            ahead = jnp.where(lane >= nz - 4, aheads[g + 1] if g < groups - 1 else 0.0, aheads[g])
            deep = jnp.where(place == 1, pltpu.roll(part, 1, 1), pltpu.roll(part, nz - 1, 1))
            rim_v[s, g] = 6.0 * part - (back + ahead + beside_rows(part) + deep)

    mark("p02b_barrier")
    pl.semaphore_wait(barrier, len(near) + len(along))
    mark("p03_halo")

    def remote(src, dst, send, recv, peer):
        return pltpu.make_async_remote_copy(
            src_ref=src, dst_ref=dst, send_sem=send, recv_sem=recv, device_id=peer, device_id_type=MESH
        )

    up = remote(edge, edge_low, edge_send.at[0], edge_recv.at[0], {"shot": shot, "depth": lax.rem(depth + 1, nd_dev)})
    down = remote(edge, edge_high, edge_send.at[1], edge_recv.at[1], {"shot": shot, "depth": lax.rem(depth + nd_dev - 1, nd_dev)})

    @pl.when(depth < nd_dev - 1)
    def _():
        up.start()

    @pl.when(depth > 0)
    def _():
        down.start()

    @pl.when(depth == 0)
    def _():
        edge_low[...] = jnp.zeros_like(edge_low)

    @pl.when(depth == nd_dev - 1)
    def _():
        edge_high[...] = jnp.zeros_like(edge_high)

    @pl.when(depth > 0)
    def _():
        up.wait_recv()

    @pl.when(depth < nd_dev - 1)
    def _():
        down.wait_recv()

    mark("p04_energy")
    for s in range(shots):
        total = jnp.where(ends, 0.0, sums[s])
        high, low = edge_high[s], edge_low[s]
        for g in range(groups):
            side = jnp.where(
                place == 1,
                pltpu.roll(high, (nz - 1 - 2 * g) % nz, 1),
                pltpu.roll(low, (nz + 1 - 2 * g) % nz, 1),
            )
            side_v[s, g] = side
            rim = rim_v[s, g] - side
            total = total + jnp.where(inner, rim * rim, 0.0)
        energy[0, s : s + 1] = jnp.sum(total, axis=0, keepdims=True)

    for i, peer in enumerate(near):
        dy, dd = (i + 1) // nd_dev, (i + 1) % nd_dev
        slot = ((ny_dev - dy) % ny_dev) * nd_dev + (nd_dev - dd) % nd_dev
        remote(energy.at[0], energy.at[slot], small_send.at[0], small_recv.at[0], peer).start()

    mark("p05_raw")
    after = lax.rem(y + 1, ny_dev)
    before = lax.rem(y + ny_dev - 1, ny_dev)
    across = lax.rem(y + ny_dev // 2, ny_dev)
    next_y = {"shot": after * nz_dev + z, "depth": depth}
    prev_y = {"shot": before * nz_dev + z, "depth": depth}

    def ends_of(packed_side, x):
        return jnp.where(ends, pltpu.roll(packed_side, lax.rem(2 * nz - 2 - 4 * lax.rem(x, group), nz), 1), 0.0)

    def raw_body(i, carry):
        for s in range(shots):
            side = side_v[s, across * per_y // group]
            for way in range(2):
                x = across * per_y + 2 * i + way
                raw_out[way, s, i] = filt[s, x] - ends_of(side, x)
        return carry

    lax.fori_loop(0, nz_dev, raw_body, 0)
    raws = [remote(raw_out.at[i], raw_in.at[i], raw_send.at[i], raw_recv.at[i], (next_y, prev_y)[i]) for i in range(2)]
    for copy in raws:
        copy.start()

    mark("p06_wait_energy")
    others = energy.at[pl.ds(1, len(near))]
    pltpu.make_async_copy(others, others, small_recv.at[0]).wait()
    mark("p07_means")
    cells = nx * ny * nz * nd_dev
    means = []
    for dy in range(ny_dev):
        both = jnp.sum(energy[dy * nd_dev : (dy + 1) * nd_dev], axis=0)
        means.append(jnp.broadcast_to(jnp.sum(both, axis=1, keepdims=True) / cells, (shots, nz)))
    peaks[0] = functools.reduce(jnp.maximum, means)
    for i, peer in enumerate(along):
        remote(peaks.at[0], peaks.at[nz_dev - 1 - i], small_send.at[1], small_recv.at[1], peer).start()
    rest = peaks.at[pl.ds(1, len(along))]
    mark("p08_wait_peak")
    pltpu.make_async_copy(rest, rest, small_recv.at[1]).wait()
    mark("p09_weights")
    peak = jnp.max(jnp.max(peaks[...], axis=0), axis=0, keepdims=True)
    scale = 1.0 / float(shots * ny_dev * nz_dev) ** 0.5
    weights = [scale / jnp.sqrt(mean + 0.5 * peak + 1.0) for mean in means]

    def weight(dy, s):
        return jnp.broadcast_to(weights[dy][s : s + 1], (ny, nz))

    for g in range(groups):
        mixed[g] = sum(weight(0, s) * side_v[s, g] for s in range(shots))

    def own(x):
        total = sum(weight(0, s) * filt[s, x] for s in range(shots))
        return total - ends_of(mixed[x // group], x)

    mark("p10_ysend")
    for copy in raws:
        copy.wait_recv()
    order = ring_order(nz_dev)
    moves = []
    for i, dz in enumerate(order):
        target = lax.rem(z + dz, nz_dev)
        for way, (peer, place_y, origin) in enumerate(((next_y, after, ny_dev - 1), (prev_y, before, 1))):
            for j in range(2):
                value = own(place_y * per_y + 2 * target + j)
                if j == way:
                    value = value + sum(weight(origin, s) * raw_in[way, s, target] for s in range(shots))
                sent[way, i, j] = value
            copy = remote(sent.at[way, i], got.at[way, i], move_send.at[way, i], move_recv.at[way, i], peer)
            copy.start()
            moves.append(copy)
    for i, dz in enumerate(order):
        target = lax.rem(z + dz, nz_dev)
        for j in range(2):
            image[i, j] = own(y * per_y + 2 * target + j)

    mark("p11_zsend")
    finals = []
    for i, dz in enumerate(order):
        for way in range(2):
            moves[2 * i + way].wait_recv()
        value = image[i] + got[0, i] + got[1, i]
        image[i] = value
        if dz:
            slot = nz_dev - 1 - dz
            copy = remote(image.at[i], arrived.at[slot], last_send.at[slot], last_recv.at[slot], along[dz - 1])
            copy.start()
            finals.append((copy, slot))
    mark("p12_zwait")
    result = value
    for copy, slot in finals:
        copy.wait_recv()
        result = result + arrived[slot]
    out[...] = result

    mark("p13_tail")
    for copy, _ in finals:
        copy.wait_send()
    for copy in moves + raws:
        copy.wait_send()
    pltpu.make_async_copy(others, others, small_send.at[0]).wait()
    pltpu.make_async_copy(rest, rest, small_send.at[1]).wait()

    @pl.when(depth < nd_dev - 1)
    def _():
        up.wait_send()

    @pl.when(depth > 0)
    def _():
        down.wait_send()

    mark(None)


def solution(mesh):
    nd_dev = mesh.shape["depth"]
    ny_dev = ROWS_Y
    nz_dev = mesh.shape["shot"] // ny_dev

    def on_device(correlation, illumination, aperture):
        shots, nx, ny, nz = correlation.shape
        per_z = nx // ny_dev // nz_dev
        assert per_z == 2 and nz == 128 and nx == 64
        dma = pltpu.SemaphoreType.DMA
        field = (ny, nz)
        return pl.pallas_call(
            functools.partial(kernel, ny_dev, nz_dev, nd_dev),
            out_shape=jax.ShapeDtypeStruct((per_z, ny, nz), F32),
            in_specs=[pl.BlockSpec(memory_space=pl.ANY)] * 3,
            out_specs=pl.BlockSpec(memory_space=pltpu.VMEM),
            scratch_shapes=[
                pltpu.SMEM((shots, 4), jnp.int32),
                pltpu.VMEM((shots, nx, *field), F32),
                pltpu.VMEM((shots, nx, *field), F32),
                pltpu.VMEM((shots, nx + 2, *field), F32),
                pltpu.VMEM((shots, nx, *field), F32),
                pltpu.VMEM((shots, *field), F32),
                pltpu.VMEM((shots, *field), F32),
                pltpu.VMEM((shots, *field), F32),
                pltpu.VMEM((shots, 2, *field), F32),
                pltpu.VMEM((shots, 2, *field), F32),
                pltpu.VMEM((2, *field), F32),
                pltpu.VMEM((ny_dev * nd_dev, shots, nz), F32),
                pltpu.VMEM((nz_dev, shots, nz), F32),
                pltpu.VMEM((2, shots, nz_dev, *field), F32),
                pltpu.VMEM((2, shots, nz_dev, *field), F32),
                pltpu.VMEM((2, nz_dev, per_z, *field), F32),
                pltpu.VMEM((2, nz_dev, per_z, *field), F32),
                pltpu.VMEM((nz_dev, per_z, *field), F32),
                pltpu.VMEM((nz_dev - 1, per_z, *field), F32),
                dma, dma((shots, PIECES, 2)),
                dma((2,)), dma((2,)), dma((2,)), dma((2,)),
                dma((2,)), dma((2,)), dma((2, nz_dev)), dma((2, nz_dev)),
                dma((nz_dev - 1,)), dma((nz_dev - 1,)),
            ],
            compiler_params=pltpu.CompilerParams(
                collective_id=0, has_side_effects=True, vmem_limit_bytes=67_043_328 - (256 << 10)
            ),
        )(aperture, correlation, illumination)

    return jax.shard_map(
        on_device,
        mesh=mesh,
        in_specs=(P("shot", None, None, "depth"), P("shot", None, None, "depth"), P("shot", None)),
        out_specs=P("shot", None, "depth"),
        check_vma=False,
    )
```

```python
import functools

import jax
import jax.numpy as jnp
from jax import lax
from jax.experimental import pallas as pl
from jax.experimental.pallas import tpu as pltpu
from jax.sharding import PartitionSpec as P

ROWS_Y = 4
PIECES = 4
UNROLL = 4
F32 = jnp.float32
MESH = pl.DeviceIdType.MESH


class Marks:
    def __init__(self):
        self.scope = None

    def __call__(self, name):
        if self.scope is not None:
            self.scope.__exit__(None, None, None)
            self.scope = None
        if name:
            self.scope = jax.named_scope(name)
            self.scope.__enter__()


def ring_order(count):
    return sorted((d for d in range(count) if 2 * d != count), key=lambda d: (-min(d, count - d), d))


def kernel(
    ny_dev, nz_dev, nd_dev,
    box_hbm, corr, illum, out,
    box, corr_v, illum_v, norm, filt, edge, edge_low, edge_high, rim_v, wrap_v, side_v, mixed,
    energy, peaks, raw_out, raw_in, cross_out, cross_in, sent, got, image, arrived,
    box_sem, load_sem, edge_send, edge_recv, small_send, small_recv,
    raw_send, raw_recv, move_send, move_recv, last_send, last_recv,
):
    shots, nx, ny, nz = filt.shape
    mark = Marks()
    mark("p00_load_signal")
    shot, depth = lax.axis_index("shot"), lax.axis_index("depth")
    y, z = shot // nz_dev, shot % nz_dev
    per_y = nx // ny_dev
    group = nz // 4
    groups = nx // group

    box_load = pltpu.make_async_copy(box_hbm, box, box_sem)
    box_load.start()
    step = nx // PIECES
    loads = []
    for c in range(PIECES):
        piece = []
        for s in range(shots):
            rows = pl.ds(c * step, step)
            piece.append(pltpu.make_async_copy(corr.at[s, rows], corr_v.at[s, rows], load_sem.at[s, c, 0]))
            piece.append(pltpu.make_async_copy(illum.at[s, rows], illum_v.at[s, rows], load_sem.at[s, c, 1]))
        for copy in piece:
            copy.start()
        loads.append(piece)

    near = []
    for dy in range(ny_dev):
        for dd in range(nd_dev):
            if dy or dd:
                near.append({
                    "shot": lax.rem(y + dy, ny_dev) * nz_dev + z,
                    "depth": lax.rem(depth + dd, nd_dev),
                })
    along = [
        {"shot": y * nz_dev + lax.rem(z + dz, nz_dev), "depth": depth} for dz in range(1, nz_dev)
    ]
    after, before, across = (lax.rem(y + d, ny_dev) for d in (1, ny_dev - 1, ny_dev // 2))
    corners = [
        {"shot": side * nz_dev + lax.rem(z + d, nz_dev), "depth": depth}
        for side, d in ((after, 1), (before, nz_dev - 1))
    ]
    barrier = pltpu.get_barrier_semaphore()
    for peer in near + along + corners:
        pl.semaphore_signal(barrier, inc=1, device_id=peer, device_id_type=MESH)

    lane = lax.broadcasted_iota(jnp.int32, (ny, nz), 1)
    row = lax.broadcasted_iota(jnp.int32, (ny, nz), 0)
    ends = (lane == 0) | (lane == nz - 1)
    top, bottom = row == 0, row == ny - 1
    column = lane // 4
    place = lax.rem(lane, 4)
    zero = jnp.zeros((ny, nz), F32)

    def beside_rows(here):
        return jnp.where(top, 0.0, pltpu.roll(here, 1, 0)) + jnp.where(bottom, 0.0, pltpu.roll(here, ny - 1, 0))

    box_load.wait()
    mark("p01_filter")
    strips = [((row >= box[s, 2]) & (row < box[s, 3])).astype(F32) for s in range(shots)]
    bounds = [(box[s, 0], box[s, 1]) for s in range(shots)]
    for s in range(shots):
        norm[s, 0] = zero
        norm[s, nx + 1] = zero

    def normalize(k, packs):
        packs = list(packs)
        for s in range(shots):
            for j in range(UNROLL):
                x = k * UNROLL + j
                inside = jnp.where((x >= bounds[s][0]) & (x < bounds[s][1]), 1.0, 0.0).astype(F32)
                value = (strips[s] * inside) * corr_v[s, x] / (illum_v[s, x] + 0.1)
                norm[s, x + 1] = value
                turned = pltpu.roll(value, lax.rem(4 * x + 2, nz), 1)
                packs[s] = jnp.where(column == lax.rem(x, group), turned, packs[s])
        return tuple(packs)

    def filter_block(k, sums):
        sums = list(sums)
        for s in range(shots):
            rows = [norm[s, k * UNROLL + i] for i in range(UNROLL + 2)]
            for j in range(UNROLL):
                here = rows[j + 1]
                beside = rows[j] + rows[j + 2] + beside_rows(here)
                beside = beside + pltpu.roll(here, 1, 1) + pltpu.roll(here, nz - 1, 1)
                value = 6.0 * here - beside
                filt[s, k * UNROLL + j] = value
                sums[s] = sums[s] + value * value
        return tuple(sums)

    blocks = nx // UNROLL
    per_piece = step // UNROLL
    packs, sums, packed = (zero,) * shots, (zero,) * shots, []
    for c in range(PIECES):
        for copy in loads[c]:
            copy.wait()
        begin = c * per_piece
        if c == 0:
            for k in range(2):
                packs = normalize(k, packs)
            begin = 2

        def body(k, carry):
            packs, sums = carry
            sums = filter_block(k - 2, sums)
            return normalize(k, packs), sums

        packs, sums = lax.fori_loop(begin, (c + 1) * per_piece, body, (packs, sums))
        if (c + 1) * step % group == 0:
            packed.append(packs)
            packs = (zero,) * shots
    for k in (blocks - 2, blocks - 1):
        sums = filter_block(k, sums)

    mark("p02_pack")
    inner = (place == 1) | (place == 2)
    for s in range(shots):
        parts = [packed[g][s] for g in range(groups)]
        edge[s] = jnp.where(inner, parts[0], pltpu.roll(parts[1], 2, 1))
        backs = [pltpu.roll(part, 4, 1) for part in parts]
        aheads = [pltpu.roll(part, nz - 4, 1) for part in parts]
        for g, part in enumerate(parts):
            back = jnp.where(lane < 4, backs[g - 1] if g else 0.0, backs[g])
            ahead = jnp.where(lane >= nz - 4, aheads[g + 1] if g < groups - 1 else 0.0, aheads[g])
            lower, higher = pltpu.roll(part, 1, 1), pltpu.roll(part, nz - 1, 1)
            deep = jnp.where(place == 1, lower, higher)
            rim_v[s, g] = 6.0 * part - (back + ahead + beside_rows(part) + deep)
            wrap_v[s, g] = jnp.where(place == 1, higher, lower)

    mark("p02b_barrier")
    pl.semaphore_wait(barrier, len(near) + len(along) + len(corners))
    mark("p03_halo")

    def remote(src, dst, send, recv, peer):
        return pltpu.make_async_remote_copy(
            src_ref=src, dst_ref=dst, send_sem=send, recv_sem=recv, device_id=peer, device_id_type=MESH
        )

    up = remote(edge, edge_low, edge_send.at[0], edge_recv.at[0], {"shot": shot, "depth": lax.rem(depth + 1, nd_dev)})
    down = remote(edge, edge_high, edge_send.at[1], edge_recv.at[1], {"shot": shot, "depth": lax.rem(depth + nd_dev - 1, nd_dev)})

    @pl.when(depth < nd_dev - 1)
    def _():
        up.start()

    @pl.when(depth > 0)
    def _():
        down.start()

    @pl.when(depth == 0)
    def _():
        edge_low[...] = jnp.zeros_like(edge_low)

    @pl.when(depth == nd_dev - 1)
    def _():
        edge_high[...] = jnp.zeros_like(edge_high)

    @pl.when(depth > 0)
    def _():
        up.wait_recv()

    @pl.when(depth < nd_dev - 1)
    def _():
        down.wait_recv()

    mark("p04_energy")
    for s in range(shots):
        total = jnp.where(ends, 0.0, sums[s])
        high, low = edge_high[s], edge_low[s]
        for g in range(groups):
            side = jnp.where(
                place == 1,
                pltpu.roll(high, (nz - 1 - 2 * g) % nz, 1),
                pltpu.roll(low, (nz + 1 - 2 * g) % nz, 1),
            )
            side_v[s, g] = side - wrap_v[s, g]
            rim = rim_v[s, g] - side
            total = total + jnp.where(inner, rim * rim, 0.0)
        energy[0, s : s + 1] = jnp.sum(total, axis=0, keepdims=True)

    for i, peer in enumerate(near):
        dy, dd = (i + 1) // nd_dev, (i + 1) % nd_dev
        slot = ((ny_dev - dy) % ny_dev) * nd_dev + (nd_dev - dd) % nd_dev
        remote(energy.at[0], energy.at[slot], small_send.at[0], small_recv.at[0], peer).start()

    mark("p05_raw")
    next_y = {"shot": after * nz_dev + z, "depth": depth}
    prev_y = {"shot": before * nz_dev + z, "depth": depth}
    next_z, prev_z = along[0], along[-1]
    order = ring_order(nz_dev)
    owners = [lax.rem(z + dz, nz_dev) for dz in order]
    opposite = lax.rem(z + nz_dev // 2, nz_dev)

    def ends_of(packed_side, x):
        return jnp.where(ends, pltpu.roll(packed_side, lax.rem(2 * nz - 2 - 4 * lax.rem(x, group), nz), 1), 0.0)

    def raw(s, x):
        return filt[s, x] - ends_of(side_v[s, x // group], x)

    chips = (y, after, before, across)
    for way in range(2):
        for s in range(shots):
            for i, chip in enumerate(chips):
                cross_out[way, s, i] = raw(s, chip * per_y + 2 * opposite + way)
    raws = []
    for way in range(2):
        straight, corner = pl.ds(0, 3), pl.ds(3, 1)
        raws.append(remote(
            cross_out.at[way, :, straight], cross_in.at[way, :, straight],
            raw_send.at[0, way], raw_recv.at[0, way], (next_z, prev_z)[way],
        ))
        raws.append(remote(
            cross_out.at[way, :, corner], cross_in.at[way, :, corner],
            raw_send.at[1, way], raw_recv.at[1, way], corners[way],
        ))
    for copy in raws:
        copy.start()
    for way in range(2):
        for s in range(shots):
            for i, owner in enumerate(owners):
                raw_out[way, s, i] = raw(s, across * per_y + 2 * owner + way)
        copy = remote(raw_out.at[way], raw_in.at[way], raw_send.at[2, way], raw_recv.at[2, way], (next_y, prev_y)[way])
        copy.start()
        raws.append(copy)

    mark("p06_wait_energy")
    others = energy.at[pl.ds(1, len(near))]
    pltpu.make_async_copy(others, others, small_recv.at[0]).wait()
    mark("p07_means")
    cells = nx * ny * nz * nd_dev
    means = []
    for dy in range(ny_dev):
        both = jnp.sum(energy[dy * nd_dev : (dy + 1) * nd_dev], axis=0)
        means.append(jnp.broadcast_to(jnp.sum(both, axis=1, keepdims=True) / cells, (shots, nz)))
    for dy in range(ny_dev):
        peaks[0, dy * shots : (dy + 1) * shots] = means[dy]
    for i, peer in enumerate(along):
        remote(peaks.at[0], peaks.at[nz_dev - 1 - i], small_send.at[1], small_recv.at[1], peer).start()
    rest = peaks.at[pl.ds(1, len(along))]
    mark("p08_wait_peak")
    pltpu.make_async_copy(rest, rest, small_recv.at[1]).wait()
    mark("p09_weights")
    peak = jnp.max(jnp.max(peaks[...], axis=0), axis=0, keepdims=True)
    scale = 1.0 / float(shots * ny_dev * nz_dev) ** 0.5
    weights = {dz: scale / jnp.sqrt(peaks[dz] + 0.5 * peak + 1.0) for dz in (0, 1, nz_dev - 1)}

    def weight(dy, dz, s):
        return jnp.broadcast_to(weights[dz][dy * shots + s : dy * shots + s + 1], (ny, nz))

    def blend(dy, dz, value):
        return sum(weight(dy, dz, s) * value(s) for s in range(shots))

    for g in range(groups):
        mixed[g] = blend(0, 0, lambda s: side_v[s, g])

    mark("p10_ysend")
    for copy in raws:
        copy.wait_recv()

    def share(i, chip, j):
        x = chips[chip] * per_y + 2 * owners[i] + j
        total = blend(0, 0, lambda s: filt[s, x]) - ends_of(mixed[x // group], x)
        if chip and j == chip - 1:
            total = total + blend((ny_dev - 1, 1)[j], 0, lambda s: raw_in[j, s, i])
        if order[i] == (nz_dev // 2 - 1, nz_dev // 2 + 1)[j]:
            total = total + blend(0, (nz_dev - 1, 1)[j], lambda s: cross_in[j, s, chip])
            if chip and j == chip - 1:
                total = total + blend((ny_dev - 1, 1)[j], (nz_dev - 1, 1)[j], lambda s: cross_in[j, s, 3])
        return total

    moves = []
    for i in range(len(order)):
        for way, peer in enumerate((next_y, prev_y)):
            for j in range(2):
                sent[way, i, j] = share(i, 1 + way, j)
            copy = remote(sent.at[way, i], got.at[way, i], move_send.at[way, i], move_recv.at[way, i], peer)
            copy.start()
            moves.append(copy)
    for i in range(len(order)):
        for j in range(2):
            image[i, j] = share(i, 0, j)

    mark("p11_zsend")
    finals = []
    for i, dz in enumerate(order):
        for way in range(2):
            moves[2 * i + way].wait_recv()
        value = image[i] + got[0, i] + got[1, i]
        image[i] = value
        if dz:
            copy = remote(image.at[i], arrived.at[i], last_send.at[i], last_recv.at[i], along[dz - 1])
            copy.start()
            finals.append(copy)
    mark("p12_zwait")
    result = value
    for i, copy in enumerate(finals):
        copy.wait_recv()
        result = result + arrived[i]
    out[...] = result

    mark("p13_tail")
    for copy in finals:
        copy.wait_send()
    for copy in moves + raws:
        copy.wait_send()
    pltpu.make_async_copy(others, others, small_send.at[0]).wait()
    pltpu.make_async_copy(rest, rest, small_send.at[1]).wait()

    @pl.when(depth < nd_dev - 1)
    def _():
        up.wait_send()

    @pl.when(depth > 0)
    def _():
        down.wait_send()

    mark(None)


def solution(mesh):
    nd_dev = mesh.shape["depth"]
    ny_dev = ROWS_Y
    nz_dev = mesh.shape["shot"] // ny_dev

    def on_device(correlation, illumination, aperture):
        shots, nx, ny, nz = correlation.shape
        per_z = nx // ny_dev // nz_dev
        assert per_z == 2 and nz == 128 and nx == 64
        dma = pltpu.SemaphoreType.DMA
        field = (ny, nz)
        chunks = len(ring_order(nz_dev))
        return pl.pallas_call(
            functools.partial(kernel, ny_dev, nz_dev, nd_dev),
            out_shape=jax.ShapeDtypeStruct((per_z, ny, nz), F32),
            in_specs=[pl.BlockSpec(memory_space=pl.ANY)] * 3,
            out_specs=pl.BlockSpec(memory_space=pltpu.VMEM),
            scratch_shapes=[
                pltpu.SMEM((shots, 4), jnp.int32),
                pltpu.VMEM((shots, nx, *field), F32),
                pltpu.VMEM((shots, nx, *field), F32),
                pltpu.VMEM((shots, nx + 2, *field), F32),
                pltpu.VMEM((shots, nx, *field), F32),
                pltpu.VMEM((shots, *field), F32),
                pltpu.VMEM((shots, *field), F32),
                pltpu.VMEM((shots, *field), F32),
                pltpu.VMEM((shots, 2, *field), F32),
                pltpu.VMEM((shots, 2, *field), F32),
                pltpu.VMEM((shots, 2, *field), F32),
                pltpu.VMEM((2, *field), F32),
                pltpu.VMEM((ny_dev * nd_dev, shots, nz), F32),
                pltpu.VMEM((nz_dev, ny_dev * shots, nz), F32),
                pltpu.VMEM((2, shots, chunks, *field), F32),
                pltpu.VMEM((2, shots, chunks, *field), F32),
                pltpu.VMEM((2, shots, 4, *field), F32),
                pltpu.VMEM((2, shots, 4, *field), F32),
                pltpu.VMEM((2, chunks, per_z, *field), F32),
                pltpu.VMEM((2, chunks, per_z, *field), F32),
                pltpu.VMEM((chunks, per_z, *field), F32),
                pltpu.VMEM((chunks - 1, per_z, *field), F32),
                dma, dma((shots, PIECES, 2)),
                dma((2,)), dma((2,)), dma((2,)), dma((2,)),
                dma((3, 2)), dma((3, 2)), dma((2, chunks)), dma((2, chunks)),
                dma((chunks - 1,)), dma((chunks - 1,)),
            ],
            compiler_params=pltpu.CompilerParams(
                collective_id=0, has_side_effects=True, vmem_limit_bytes=32 << 20
            ),
        )(*(pltpu.with_memory_space_constraint(a, pltpu.HBM) for a in (aperture, correlation, illumination)))

    return jax.shard_map(
        on_device,
        mesh=mesh,
        in_specs=(P("shot", None, None, "depth"), P("shot", None, None, "depth"), P("shot", None)),
        out_specs=P("shot", None, "depth"),
        check_vma=False,
    )
```

```python
import functools

import jax
import jax.numpy as jnp
from jax import lax
from jax.experimental import pallas as pl
from jax.experimental.pallas import tpu as pltpu
from jax.sharding import PartitionSpec as P

ROWS_Y = 4
PIECES = 4
NORM_ROWS = 16
FILTER_ROWS = 16
PAD = 8
ORDER = (0, 1, 2, 3, 7, 6, 5, 4)
F32 = jnp.float32
MESH = pl.DeviceIdType.MESH


class Marks:
    def __init__(self):
        self.scope = None

    def __call__(self, name):
        if self.scope is not None:
            self.scope.__exit__(None, None, None)
            self.scope = None
        if name:
            self.scope = jax.named_scope(name)
            self.scope.__enter__()


def kernel(
    ny_dev, nz_dev, nd_dev,
    box_hbm, corr, illum, out,
    box, corr_v, illum_v, norm, filt, edge, edge_low, edge_high, rim_v, wrap_v, side_v, mixed,
    energy, peaks, raw_out, raw_in, cross_out, cross_in, cross_sum, sent, got, image, arrived,
    box_sem, load_sem, edge_send, edge_recv, small_send, small_recv,
    raw_send, raw_recv, move_send, move_recv, last_send, last_recv,
):
    shots, nx, ny, nz = filt.shape
    mark = Marks()
    mark("p00_load_signal")
    shot, depth = lax.axis_index("shot"), lax.axis_index("depth")
    y, z = shot // nz_dev, shot % nz_dev
    per_y = nx // ny_dev
    group = nz // 4
    groups = nx // group

    box_load = pltpu.make_async_copy(box_hbm, box, box_sem)
    box_load.start()
    step = nx // PIECES
    loads = []
    for c in range(PIECES):
        piece = []
        for s in range(shots):
            rows = pl.ds(c * step, step)
            piece.append(pltpu.make_async_copy(corr.at[s, rows], corr_v.at[s, rows], load_sem.at[s, c, 0]))
            piece.append(pltpu.make_async_copy(illum.at[s, rows], illum_v.at[s, rows], load_sem.at[s, c, 1]))
        loads.append(piece)
    for copy in loads[0]:
        copy.start()

    near = []
    for dy in range(ny_dev):
        for dd in range(nd_dev):
            if dy or dd:
                near.append({
                    "shot": lax.rem(y + dy, ny_dev) * nz_dev + z,
                    "depth": lax.rem(depth + dd, nd_dev),
                })
    along = [
        {"shot": y * nz_dev + lax.rem(z + dz, nz_dev), "depth": depth} for dz in range(1, nz_dev)
    ]
    after, before, across = (lax.rem(y + d, ny_dev) for d in (1, ny_dev - 1, ny_dev // 2))
    corners = [
        {"shot": side * nz_dev + lax.rem(z + d, nz_dev), "depth": depth}
        for side, d in ((after, 1), (before, nz_dev - 1))
    ]
    barrier = pltpu.get_barrier_semaphore()
    for peer in near + along + corners:
        pl.semaphore_signal(barrier, inc=1, device_id=peer, device_id_type=MESH)
    for piece in loads[1:]:
        for copy in piece:
            copy.start()

    lane = lax.broadcasted_iota(jnp.int32, (ny, nz), 1)
    row = lax.broadcasted_iota(jnp.int32, (ny, nz), 0)
    ends = (lane == 0) | (lane == nz - 1)
    top, bottom = row == 0, row == ny - 1
    column = lane // 4
    place = lax.rem(lane, 4)
    zero = jnp.zeros((ny, nz), F32)

    def beside_rows(here):
        return jnp.where(top, 0.0, pltpu.roll(here, 1, 0)) + jnp.where(bottom, 0.0, pltpu.roll(here, ny - 1, 0))

    strips = [((row >= box[s, 2]) & (row < box[s, 3])).astype(F32) for s in range(shots)]
    bounds = [(box[s, 0], box[s, 1]) for s in range(shots)]
    blank = jnp.zeros((PAD, nz), F32)

    def clear(x, carry):
        for s in range(shots):
            norm[s, x, :PAD] = blank
            norm[s, x, PAD + ny :] = blank
        return carry

    lax.fori_loop(1, nx + 1, clear, 0)
    for s in range(shots):
        for x in (0, nx + 1):
            norm[s, x] = jnp.zeros((ny + 2 * PAD, nz), F32)
    box_load.wait()
    strips = [((row >= box[s, 2]) & (row < box[s, 3])).astype(F32) for s in range(shots)]
    bounds = [(box[s, 0], box[s, 1]) for s in range(shots)]

    def normalize(k, packs):
        packs = list(packs)
        for s in range(shots):
            for j in range(NORM_ROWS):
                x = k * NORM_ROWS + j
                inside = jnp.where((x >= bounds[s][0]) & (x < bounds[s][1]), 1.0, 0.0).astype(F32)
                value = (strips[s] * inside) * corr_v[s, x] / (illum_v[s, x] + 0.1)
                norm[s, x + 1, PAD : PAD + ny] = value
                turned = pltpu.roll(value, lax.rem(4 * x + 2, nz), 1)
                packs[s] = jnp.where(column == lax.rem(x, group), turned, packs[s])
        return tuple(packs)

    def filter_block(k, sums):
        sums = list(sums)
        for s in range(shots):
            base = k * FILTER_ROWS
            rows = [norm[s, base + i, PAD : PAD + ny] for i in range(FILTER_ROWS + 2)]
            for j in range(FILTER_ROWS):
                here = rows[j + 1]
                beside = rows[j] + rows[j + 2] + (norm[s, base + j + 1, pl.ds(PAD - 1 + lax.min(k, 0), ny)] + norm[s, base + j + 1, pl.ds(PAD + 1 + lax.min(k, 0), ny)])
                beside = beside + pltpu.roll(here, 1, 1) + pltpu.roll(here, nz - 1, 1)
                value = 6.0 * here - beside
                filt[s, base + j] = value
                sums[s] = sums[s] + value * value
        return tuple(sums)

    packs, packed = (zero,) * shots, []
    for c in range(PIECES):
        mark(f"p01_w{c}")
        for copy in loads[c]:
            copy.wait()
        mark(f"p01_x{c}")
        blocks = step // NORM_ROWS
        packs = lax.fori_loop(c * blocks, (c + 1) * blocks, normalize, packs)
        if (c + 1) * step % group == 0:
            packed.append(packs)
            packs = (zero,) * shots

    mark("p02_pack")
    inner = (place == 1) | (place == 2)
    for s in range(shots):
        edge[s] = jnp.where(inner, packed[0][s], pltpu.roll(packed[1][s], 2, 1))

    mark("p02b_barrier")
    pl.semaphore_wait(barrier, len(near) + len(along) + len(corners))
    mark("p03_halo")

    def remote(src, dst, send, recv, peer):
        return pltpu.make_async_remote_copy(
            src_ref=src, dst_ref=dst, send_sem=send, recv_sem=recv, device_id=peer, device_id_type=MESH
        )

    up = remote(edge, edge_low, edge_send.at[0], edge_recv.at[0], {"shot": shot, "depth": lax.rem(depth + 1, nd_dev)})
    down = remote(edge, edge_high, edge_send.at[1], edge_recv.at[1], {"shot": shot, "depth": lax.rem(depth + nd_dev - 1, nd_dev)})

    @pl.when(depth < nd_dev - 1)
    def _():
        up.start()

    @pl.when(depth > 0)
    def _():
        down.start()

    @pl.when(depth == 0)
    def _():
        edge_low[...] = jnp.zeros_like(edge_low)

    @pl.when(depth == nd_dev - 1)
    def _():
        edge_high[...] = jnp.zeros_like(edge_high)

    mark("p03_filter")
    sums = lax.fori_loop(0, nx // FILTER_ROWS, filter_block, (zero,) * shots)

    mark("p03a_rim")
    for s in range(shots):
        parts = [packed[g][s] for g in range(groups)]
        backs = [pltpu.roll(part, 4, 1) for part in parts]
        aheads = [pltpu.roll(part, nz - 4, 1) for part in parts]
        for g, part in enumerate(parts):
            back = jnp.where(lane < 4, backs[g - 1] if g else 0.0, backs[g])
            ahead = jnp.where(lane >= nz - 4, aheads[g + 1] if g < groups - 1 else 0.0, aheads[g])
            lower, higher = pltpu.roll(part, 1, 1), pltpu.roll(part, nz - 1, 1)
            deep = jnp.where(place == 1, lower, higher)
            rim_v[s, g] = 6.0 * part - (back + ahead + beside_rows(part) + deep)
            wrap_v[s, g] = jnp.where(place == 1, higher, lower)

    mark("p03w_halo")
    @pl.when(depth > 0)
    def _():
        up.wait_recv()

    @pl.when(depth < nd_dev - 1)
    def _():
        down.wait_recv()

    mark("p04_energy")
    for s in range(shots):
        total = jnp.where(ends, 0.0, sums[s])
        high, low = edge_high[s], edge_low[s]
        for g in range(groups):
            side = jnp.where(
                place == 1,
                pltpu.roll(high, (nz - 1 - 2 * g) % nz, 1),
                pltpu.roll(low, (nz + 1 - 2 * g) % nz, 1),
            )
            side_v[s, g] = side - wrap_v[s, g]
            rim = rim_v[s, g] - side
            total = total + jnp.where(inner, rim * rim, 0.0)
        energy[0, s : s + 1] = jnp.sum(total, axis=0, keepdims=True)

    for i, peer in enumerate(near):
        dy, dd = (i + 1) // nd_dev, (i + 1) % nd_dev
        slot = ((ny_dev - dy) % ny_dev) * nd_dev + (nd_dev - dd) % nd_dev
        remote(energy.at[0], energy.at[slot], small_send.at[0], small_recv.at[0], peer).start()

    mark("p05_raw")
    next_y = {"shot": after * nz_dev + z, "depth": depth}
    prev_y = {"shot": before * nz_dev + z, "depth": depth}
    next_z, prev_z = along[0], along[-1]
    opposite = lax.rem(z + nz_dev // 2, nz_dev)
    def position(owner):
        return sum(jnp.where(owner == other, k, 0).astype(jnp.int32) for k, other in enumerate(ORDER))

    gap = position(opposite)
    owners = [jnp.where(i >= gap, ORDER[i + 1], ORDER[i]).astype(jnp.int32) for i in range(nz_dev - 1)]
    reach = [lax.rem(owner - z + nz_dev, nz_dev) for owner in owners]

    def ends_of(packed_side, x):
        return jnp.where(ends, pltpu.roll(packed_side, lax.rem(2 * nz - 2 - 4 * lax.rem(x, group), nz), 1), 0.0)

    def raw(s, x):
        return filt[s, x] - ends_of(side_v[s, x // group], x)

    chips = (y, after, before, across)
    for way in range(2):
        for s in range(shots):
            for i, chip in enumerate(chips):
                cross_out[way, s, i] = raw(s, chip * per_y + 2 * opposite + way)
    raws = []
    for way in range(2):
        straight, corner = pl.ds(0, 3), pl.ds(3, 1)
        raws.append(remote(
            cross_out.at[way, :, straight], cross_in.at[way, :, straight],
            raw_send.at[0, way], raw_recv.at[0, way], (next_z, prev_z)[way],
        ))
        raws.append(remote(
            cross_out.at[way, :, corner], cross_in.at[way, :, corner],
            raw_send.at[1, way], raw_recv.at[1, way], corners[way],
        ))
    for copy in raws:
        copy.start()
    for way in range(2):
        for s in range(shots):
            for i, owner in enumerate(owners):
                raw_out[way, s, i] = raw(s, across * per_y + 2 * owner + way)
        copy = remote(raw_out.at[way], raw_in.at[way], raw_send.at[2, way], raw_recv.at[2, way], (next_y, prev_y)[way])
        copy.start()
        raws.append(copy)

    mark("p06_wait_energy")
    others = energy.at[pl.ds(1, len(near))]
    pltpu.make_async_copy(others, others, small_recv.at[0]).wait()
    mark("p07_means")
    cells = nx * ny * nz * nd_dev
    means = []
    for dy in range(ny_dev):
        both = jnp.sum(energy[dy * nd_dev : (dy + 1) * nd_dev], axis=0)
        means.append(jnp.broadcast_to(jnp.sum(both, axis=1, keepdims=True) / cells, (shots, nz)))
    for dy in range(ny_dev):
        peaks[0, dy * shots : (dy + 1) * shots] = means[dy]
    for i, peer in enumerate(along):
        remote(peaks.at[0], peaks.at[nz_dev - 1 - i], small_send.at[1], small_recv.at[1], peer).start()
    rest = peaks.at[pl.ds(1, len(along))]
    mark("p08_wait_peak")
    pltpu.make_async_copy(rest, rest, small_recv.at[1]).wait()
    mark("p09_weights")
    peak = jnp.max(jnp.max(peaks[...], axis=0), axis=0, keepdims=True)
    scale = 1.0 / float(shots * ny_dev * nz_dev) ** 0.5
    weights = {dz: scale / jnp.sqrt(peaks[dz] + 0.5 * peak + 1.0) for dz in (0, 1, nz_dev - 1)}

    def weight(dy, dz, s):
        return jnp.broadcast_to(weights[dz][dy * shots + s : dy * shots + s + 1], (ny, nz))

    def blend(dy, dz, value):
        return sum(weight(dy, dz, s) * value(s) for s in range(shots))

    for g in range(groups):
        mixed[g] = blend(0, 0, lambda s: side_v[s, g])

    mark("p10_ysend")
    for copy in raws:
        copy.wait_recv()

    def share(i, chip, j):
        x = chips[chip] * per_y + 2 * owners[i] + j
        total = blend(0, 0, lambda s: filt[s, x]) - ends_of(mixed[x // group], x)
        if chip and j == chip - 1:
            total = total + blend((ny_dev - 1, 1)[j], 0, lambda s: raw_in[j, s, i])
        beyond = jnp.where(reach[i] == (nz_dev // 2 - 1, nz_dev // 2 + 1)[j], 1.0, 0.0).astype(F32)
        return total + beyond * cross_sum[j, chip]

    for j in range(2):
        for chip in range(3):
            total = blend(0, (nz_dev - 1, 1)[j], lambda s: cross_in[j, s, chip])
            if chip == j + 1:
                total = total + blend((ny_dev - 1, 1)[j], (nz_dev - 1, 1)[j], lambda s: cross_in[j, s, 3])
            cross_sum[j, chip] = total

    moves = []
    for i in range(len(owners)):
        for way, peer in enumerate((next_y, prev_y)):
            for j in range(2):
                sent[way, i, j] = share(i, 1 + way, j)
            copy = remote(sent.at[way, i], got.at[way, i], move_send.at[way, i], move_recv.at[way, i], peer)
            moves.append(copy)
            copy.start()
    for i in range(len(owners)):
        for j in range(2):
            image[i, j] = share(i, 0, j)

    mark("p10b_turn")

    mark("p11_zsend")
    def final(i):
        slot = lax.rem(z - owners[i] + nz_dev, nz_dev)
        peer = {"shot": y * nz_dev + owners[i], "depth": depth}
        return remote(image.at[i], arrived.at[slot], last_send.at[i], last_recv.at[slot], peer)

    for i, owner in enumerate(owners):
        for way in range(2):
            moves[2 * i + way].wait_recv()
        image[i] = image[i] + got[0, i] + got[1, i]

        @pl.when(owner != z)
        def _(i=i):
            final(i).start()

    mark("p12_zwait")
    result = image[position(z) - jnp.where(position(z) > gap, 1, 0).astype(jnp.int32)]
    for dz in sorted(range(1, nz_dev), key=lambda d: min(d, nz_dev - d)):
        if 2 * dz != nz_dev:
            pltpu.make_async_copy(arrived.at[dz], arrived.at[dz], last_recv.at[dz]).wait()
            result = result + arrived[dz]
    out[...] = result

    mark("p13_tail")
    for i, owner in enumerate(owners):

        @pl.when(owner != z)
        def _(i=i):
            final(i).wait_send()

    for copy in raws + moves:
        copy.wait_send()

    pltpu.make_async_copy(others, others, small_send.at[0]).wait()
    pltpu.make_async_copy(rest, rest, small_send.at[1]).wait()

    @pl.when(depth < nd_dev - 1)
    def _():
        up.wait_send()

    @pl.when(depth > 0)
    def _():
        down.wait_send()

    mark(None)


def solution(mesh):
    nd_dev = mesh.shape["depth"]
    ny_dev = ROWS_Y
    nz_dev = mesh.shape["shot"] // ny_dev

    def on_device(correlation, illumination, aperture):
        shots, nx, ny, nz = correlation.shape
        per_z = nx // ny_dev // nz_dev
        assert per_z == 2 and nz == 128 and nx == 64
        dma = pltpu.SemaphoreType.DMA
        field = (ny, nz)
        chunks = nz_dev - 1
        return pl.pallas_call(
            functools.partial(kernel, ny_dev, nz_dev, nd_dev),
            out_shape=jax.ShapeDtypeStruct((per_z, ny, nz), F32),
            in_specs=[pl.BlockSpec(memory_space=pl.ANY)] * 3,
            out_specs=pl.BlockSpec(memory_space=pltpu.VMEM),
            scratch_shapes=[
                pltpu.SMEM((shots, 4), jnp.int32),
                pltpu.VMEM((shots, nx, *field), F32),
                pltpu.VMEM((shots, nx, *field), F32),
                pltpu.VMEM((shots, nx + 2, ny + 2 * PAD, nz), F32),
                pltpu.VMEM((shots, nx, *field), F32),
                pltpu.VMEM((shots, *field), F32),
                pltpu.VMEM((shots, *field), F32),
                pltpu.VMEM((shots, *field), F32),
                pltpu.VMEM((shots, 2, *field), F32),
                pltpu.VMEM((shots, 2, *field), F32),
                pltpu.VMEM((shots, 2, *field), F32),
                pltpu.VMEM((2, *field), F32),
                pltpu.VMEM((ny_dev * nd_dev, shots, nz), F32),
                pltpu.VMEM((nz_dev, ny_dev * shots, nz), F32),
                pltpu.VMEM((2, shots, chunks, *field), F32),
                pltpu.VMEM((2, shots, chunks, *field), F32),
                pltpu.VMEM((2, shots, 4, *field), F32),
                pltpu.VMEM((2, shots, 4, *field), F32),
                pltpu.VMEM((2, 3, *field), F32),
                pltpu.VMEM((2, chunks, per_z, *field), F32),
                pltpu.VMEM((2, chunks, per_z, *field), F32),
                pltpu.VMEM((chunks, per_z, *field), F32),
                pltpu.VMEM((nz_dev, per_z, *field), F32),
                dma, dma((shots, PIECES, 2)),
                dma((2,)), dma((2,)), dma((2,)), dma((2,)),
                dma((3, 2)), dma((3, 2)), dma((2, chunks)), dma((2, chunks)),
                dma((chunks,)), dma((nz_dev,)),
            ],
            compiler_params=pltpu.CompilerParams(
                collective_id=0, has_side_effects=True, vmem_limit_bytes=32 << 20
            ),
        )(*(pltpu.with_memory_space_constraint(a, pltpu.HBM) for a in (aperture, correlation, illumination)))

    return jax.shard_map(
        on_device,
        mesh=mesh,
        in_specs=(P("shot", None, None, "depth"), P("shot", None, None, "depth"), P("shot", None)),
        out_specs=P("shot", None, "depth"),
        check_vma=False,
    )
```

```python
import functools

import jax
import jax.numpy as jnp
from jax import lax
from jax.experimental import pallas as pl
from jax.experimental.pallas import tpu as pltpu
from jax.sharding import PartitionSpec as P

ROWS_Y = 4
PIECES = 4
NORM_ROWS = 16
FILTER_ROWS = 16
PAD = 8
REACH = (-3, 3, 1, -1, 0)
F32 = jnp.float32
MESH = pl.DeviceIdType.MESH


class Marks:
    def __init__(self):
        self.scope = None

    def __call__(self, name):
        if self.scope is not None:
            self.scope.__exit__(None, None, None)
            self.scope = None
        if name:
            self.scope = jax.named_scope(name)
            self.scope.__enter__()


def kernel(
    ny_dev, nz_dev, nd_dev,
    box_hbm, corr, illum, out,
    box, corr_v, illum_v, norm, filt, edge, edge_low, edge_high, rim_v, wrap_v, side_v, mixed,
    energy, peaks, raw_out, raw_in, cross_out, cross_in, beside_out, beside_in, corner_out, corner_in, direct, sent, got, image, arrived,
    box_sem, load_sem, edge_send, edge_recv, small_send, small_recv,
    raw_send, raw_recv, move_send, move_recv, last_send, last_recv,
):
    shots, nx, ny, nz = filt.shape
    mark = Marks()
    mark("p00_load_signal")
    shot, depth = lax.axis_index("shot"), lax.axis_index("depth")
    y, z = shot // nz_dev, shot % nz_dev
    per_y = nx // ny_dev
    group = nz // 4
    groups = nx // group

    box_load = pltpu.make_async_copy(box_hbm, box, box_sem)
    box_load.start()
    step = nx // PIECES
    loads = []
    for c in range(PIECES):
        piece = []
        for s in range(shots):
            rows = pl.ds(c * step, step)
            piece.append(pltpu.make_async_copy(corr.at[s, rows], corr_v.at[s, rows], load_sem.at[s, c, 0]))
            piece.append(pltpu.make_async_copy(illum.at[s, rows], illum_v.at[s, rows], load_sem.at[s, c, 1]))
        loads.append(piece)
    for copy in loads[0]:
        copy.start()

    near = []
    for dy in range(ny_dev):
        for dd in range(nd_dev):
            if dy or dd:
                near.append({
                    "shot": lax.rem(y + dy, ny_dev) * nz_dev + z,
                    "depth": lax.rem(depth + dd, nd_dev),
                })
    along = [
        {"shot": y * nz_dev + lax.rem(z + dz, nz_dev), "depth": depth} for dz in range(1, nz_dev)
    ]
    after, before, across = (lax.rem(y + d, ny_dev) for d in (1, ny_dev - 1, ny_dev // 2))
    corners = [
        {"shot": side * nz_dev + lax.rem(z + d, nz_dev), "depth": depth}
        for d in (1, nz_dev - 1)
        for side in (after, before)
    ]
    barrier = pltpu.get_barrier_semaphore()
    core = lax.rem(depth, 2)
    cross_core = [{"shot": peer["shot"], "depth": depth + 1 - 2 * core} for peer in along]
    for peer in near + along + cross_core + corners:
        pl.semaphore_signal(barrier, inc=1, device_id=peer, device_id_type=MESH)
    for piece in loads[1:]:
        for copy in piece:
            copy.start()

    lane = lax.broadcasted_iota(jnp.int32, (ny, nz), 1)
    row = lax.broadcasted_iota(jnp.int32, (ny, nz), 0)
    ends = (lane == 0) | (lane == nz - 1)
    top, bottom = row == 0, row == ny - 1
    column = lane // 4
    place = lax.rem(lane, 4)
    zero = jnp.zeros((ny, nz), F32)

    def beside_rows(here):
        return jnp.where(top, 0.0, pltpu.roll(here, 1, 0)) + jnp.where(bottom, 0.0, pltpu.roll(here, ny - 1, 0))

    strips = [((row >= box[s, 2]) & (row < box[s, 3])).astype(F32) for s in range(shots)]
    bounds = [(box[s, 0], box[s, 1]) for s in range(shots)]
    blank = jnp.zeros((PAD, nz), F32)

    def clear(x, carry):
        for s in range(shots):
            norm[s, x, :PAD] = blank
            norm[s, x, PAD + ny :] = blank
        return carry

    lax.fori_loop(1, nx + 1, clear, 0)
    for s in range(shots):
        for x in (0, nx + 1):
            norm[s, x] = jnp.zeros((ny + 2 * PAD, nz), F32)
    box_load.wait()
    strips = [((row >= box[s, 2]) & (row < box[s, 3])).astype(F32) for s in range(shots)]
    bounds = [(box[s, 0], box[s, 1]) for s in range(shots)]

    def normalize(k, packs):
        packs = list(packs)
        for s in range(shots):
            for j in range(NORM_ROWS):
                x = k * NORM_ROWS + j
                inside = jnp.where((x >= bounds[s][0]) & (x < bounds[s][1]), 1.0, 0.0).astype(F32)
                value = (strips[s] * inside) * corr_v[s, x] / (illum_v[s, x] + 0.1)
                norm[s, x + 1, PAD : PAD + ny] = value
                turned = pltpu.roll(value, lax.rem(4 * x + 2, nz), 1)
                packs[s] = jnp.where(column == lax.rem(x, group), turned, packs[s])
        return tuple(packs)

    def filter_block(k, sums):
        sums = list(sums)
        for s in range(shots):
            base = k * FILTER_ROWS
            rows = [norm[s, base + i, PAD : PAD + ny] for i in range(FILTER_ROWS + 2)]
            for j in range(FILTER_ROWS):
                here = rows[j + 1]
                beside = rows[j] + rows[j + 2] + (norm[s, base + j + 1, pl.ds(PAD - 1 + lax.min(k, 0), ny)] + norm[s, base + j + 1, pl.ds(PAD + 1 + lax.min(k, 0), ny)])
                beside = beside + pltpu.roll(here, 1, 1) + pltpu.roll(here, nz - 1, 1)
                value = 6.0 * here - beside
                filt[s, base + j] = value
                sums[s] = sums[s] + value * value
        return tuple(sums)

    packs, packed = (zero,) * shots, []
    for c in range(PIECES):
        mark(f"p01_w{c}")
        for copy in loads[c]:
            copy.wait()
        mark(f"p01_x{c}")
        blocks = step // NORM_ROWS
        packs = lax.fori_loop(c * blocks, (c + 1) * blocks, normalize, packs)
        if (c + 1) * step % group == 0:
            packed.append(packs)
            packs = (zero,) * shots

    mark("p02_pack")
    inner = (place == 1) | (place == 2)
    rims = [jnp.where(inner, packed[0][s], pltpu.roll(packed[1][s], 2, 1)) for s in range(shots)]
    odd = lax.rem(lane, 2) == 1
    edge[0] = jnp.where(odd, rims[0], pltpu.roll(rims[1], 1, 1))
    edge[1] = jnp.where(odd, pltpu.roll(rims[1], nz - 1, 1), rims[0])

    mark("p02b_barrier")
    pl.semaphore_wait(barrier, len(near) + len(along) + len(cross_core) + len(corners))
    mark("p03_halo")

    def remote(src, dst, send, recv, peer):
        return pltpu.make_async_remote_copy(
            src_ref=src, dst_ref=dst, send_sem=send, recv_sem=recv, device_id=peer, device_id_type=MESH
        )

    up = remote(edge.at[0], edge_low, edge_send.at[0], edge_recv.at[0], {"shot": shot, "depth": lax.rem(depth + 1, nd_dev)})
    down = remote(edge.at[1], edge_high, edge_send.at[1], edge_recv.at[1], {"shot": shot, "depth": lax.rem(depth + nd_dev - 1, nd_dev)})

    @pl.when(depth < nd_dev - 1)
    def _():
        up.start()

    @pl.when(depth > 0)
    def _():
        down.start()

    @pl.when(depth == 0)
    def _():
        edge_low[...] = jnp.zeros_like(edge_low)

    @pl.when(depth == nd_dev - 1)
    def _():
        edge_high[...] = jnp.zeros_like(edge_high)

    mark("p03_filter")
    sums = lax.fori_loop(0, nx // FILTER_ROWS, filter_block, (zero,) * shots)

    mark("p03a_rim")
    for s in range(shots):
        parts = [packed[g][s] for g in range(groups)]
        backs = [pltpu.roll(part, 4, 1) for part in parts]
        aheads = [pltpu.roll(part, nz - 4, 1) for part in parts]
        for g, part in enumerate(parts):
            back = jnp.where(lane < 4, backs[g - 1] if g else 0.0, backs[g])
            ahead = jnp.where(lane >= nz - 4, aheads[g + 1] if g < groups - 1 else 0.0, aheads[g])
            lower, higher = pltpu.roll(part, 1, 1), pltpu.roll(part, nz - 1, 1)
            deep = jnp.where(place == 1, lower, higher)
            rim_v[s, g] = 6.0 * part - (back + ahead + beside_rows(part) + deep)
            wrap_v[s, g] = jnp.where(place == 1, higher, lower)

    mark("p03w_halo")
    @pl.when(depth > 0)
    def _():
        up.wait_recv()

    @pl.when(depth < nd_dev - 1)
    def _():
        down.wait_recv()

    mark("p04_energy")
    for s in range(shots):
        total = jnp.where(ends, 0.0, sums[s])
        high, low = edge_high[...], edge_low[...]
        for g in range(groups):
            side = jnp.where(
                place == 1,
                pltpu.roll(high, (nz - 1 - 2 * g + s) % nz, 1),
                pltpu.roll(low, (nz + 1 - 2 * g - s) % nz, 1),
            )
            side_v[s, g] = side - wrap_v[s, g]
            rim = rim_v[s, g] - side
            total = total + jnp.where(inner, rim * rim, 0.0)
        energy[0, s : s + 1] = jnp.sum(total, axis=0, keepdims=True)

    def span(i):
        dy, dd = (i + 1) // nd_dev, (i + 1) % nd_dev
        return min(dy, ny_dev - dy) + min(dd, nd_dev - dd) / 2

    for i in sorted(range(len(near)), key=span, reverse=True):
        dy, dd = (i + 1) // nd_dev, (i + 1) % nd_dev
        peer = near[i]
        slot = ((ny_dev - dy) % ny_dev) * nd_dev + (nd_dev - dd) % nd_dev
        remote(energy.at[0], energy.at[slot], small_send.at[0], small_recv.at[0], peer).start()

    mark("p05_raw")
    next_y = {"shot": after * nz_dev + z, "depth": depth}
    prev_y = {"shot": before * nz_dev + z, "depth": depth}
    next_z, prev_z = along[0], along[-1]
    owners = [lax.rem(z + nz_dev + dz, nz_dev) for dz in REACH]
    opposite = lax.rem(z + nz_dev // 2, nz_dev)
    seconds = [lax.rem(z + 2, nz_dev), lax.rem(z + nz_dev - 2, nz_dev)]

    def ends_of(packed_side, x):
        return jnp.where(ends, pltpu.roll(packed_side, lax.rem(2 * nz - 2 - 4 * lax.rem(x, group), nz), 1), 0.0)

    def raw(s, x):
        return filt[s, x] - ends_of(side_v[s, x // group], x)

    chips = (y, after, before)
    raws = []

    def push(out_ref, in_ref, index, peer):
        copy = remote(out_ref, in_ref, raw_send.at[index], raw_recv.at[index], peer)
        copy.start()
        raws.append(copy)

    for way in range(2):
        for s in range(shots):
            for i, chip in enumerate(chips):
                cross_out[way, s, i] = raw(s, chip * per_y + 2 * opposite + way)
    for way in range(2):
        push(cross_out.at[way], cross_in.at[way], way, (next_z, prev_z)[way])
    for way in range(2):
        for s in range(shots):
            for i, owner in enumerate(owners):
                raw_out[way, s, i] = raw(s, across * per_y + 2 * owner + way)
    for way in range(2):
        push(raw_out.at[way], raw_in.at[way], 2 + way, (next_y, prev_y)[way])
    for way in range(2):
        for j in range(2):
            for s in range(shots):
                for i, chip in enumerate(chips[1:]):
                    beside_out[way, j, s, i] = raw(s, chip * per_y + 2 * seconds[way] + j)
    for way in range(2):
        for j in range(2):
            for s in range(shots):
                corner_out[2 * way + j, 0, s] = raw(s, across * per_y + 2 * seconds[way] + j)
                if j == way:
                    corner_out[2 * way + j, 1, s] = raw(s, across * per_y + 2 * opposite + j)
    for k in range(4):
        part = pl.ds(0, 2 if k in (0, 3) else 1)
        push(corner_out.at[k, part], corner_in.at[k, part], 6 + k, corners[k])

    mark("p06_wait_energy")
    others = energy.at[pl.ds(1, len(near))]
    pltpu.make_async_copy(others, others, small_recv.at[0]).wait()
    mark("p07_means")
    cells = nx * ny * nz * nd_dev
    means = []
    for dy in range(ny_dev):
        both = jnp.sum(energy[dy * nd_dev : (dy + 1) * nd_dev], axis=0)
        means.append(jnp.broadcast_to(jnp.sum(both, axis=1, keepdims=True) / cells, (shots, nz)))
    for dy in range(ny_dev):
        peaks[0, dy * shots : (dy + 1) * shots] = means[dy]

    @pl.when(core == 1)
    def _():
        for peers in (cross_core, along):
            for i, peer in enumerate(peers):
                remote(peaks.at[0], peaks.at[nz_dev - 1 - i], small_send.at[1], small_recv.at[1], peer).start()

    for way in range(2):
        push(beside_out.at[way], beside_in.at[way], 4 + way, (next_z, prev_z)[way])
    rest = peaks.at[pl.ds(1, len(along))]
    mark("p08_wait_peak")
    pltpu.make_async_copy(rest, rest, small_recv.at[1]).wait()
    mark("p09_weights")
    peak = jnp.max(jnp.max(peaks[...], axis=0), axis=0, keepdims=True)
    scale = 1.0 / float(shots * ny_dev * nz_dev) ** 0.5
    weights = {dz: scale / jnp.sqrt(peaks[dz] + 0.5 * peak + 1.0) for dz in (0, 1, nz_dev - 1)}

    def weight(dy, dz, s):
        return jnp.broadcast_to(weights[dz][dy * shots + s : dy * shots + s + 1], (ny, nz))

    def blend(dy, dz, value):
        return sum(weight(dy, dz, s) * value(s) for s in range(shots))

    for g in range(groups):
        mixed[g] = blend(0, 0, lambda s: side_v[s, g])

    mark("p10_ysend")
    for copy in raws[:8]:
        copy.wait_recv()

    low, high = nz_dev - 1, 1
    behind, ahead = ny_dev - 1, 1

    def share(i, chip, j):
        x = chips[chip] * per_y + 2 * owners[i] + j
        total = blend(0, 0, lambda s: filt[s, x]) - ends_of(mixed[x // group], x)
        onward = chip and j == chip - 1
        side = (behind, ahead)[j]
        if onward:
            total = total + blend(side, 0, lambda s: raw_in[j, s, i])
        if REACH[i] == (3, -3)[j]:
            total = total + blend(0, (low, high)[j], lambda s: cross_in[j, s, chip])
            if onward:
                total = total + blend(side, (low, high)[j], lambda s: corner_in[3 * j, 1, s])
        if REACH[i] in (1, -1):
            way = (1, -1).index(REACH[i])
            if chip:
                total = total + blend(0, (low, high)[way], lambda s: beside_in[way, j, s, chip - 1])
            if onward:
                total = total + blend(side, (low, high)[way], lambda s: corner_in[2 * way + j, 0, s])
        return total

    finals = []
    for way in range(2):
        for j in range(2):
            x = y * per_y + 2 * seconds[way] + j
            direct[way, j] = blend(0, 0, lambda s: filt[s, x]) - ends_of(mixed[x // group], x)
        slot = len(REACH) + way
        copy = remote(direct.at[way], arrived.at[slot], last_send.at[slot], last_recv.at[slot], along[(1, nz_dev - 3)[way]])
        copy.start()
        finals.append((copy, slot))

    moves = []
    for i in range(len(owners)):
        if i == min(REACH.index(1), REACH.index(-1)):
            for copy in raws[8:]:
                copy.wait_recv()
        for way, peer in enumerate((next_y, prev_y)):
            for j in range(2):
                sent[way, i, j] = share(i, 1 + way, j)
            copy = remote(sent.at[way, i], got.at[way, i], move_send.at[way, i], move_recv.at[way, i], peer)
            moves.append(copy)
            copy.start()
    for i in range(len(owners)):
        for j in range(2):
            image[i, j] = share(i, 0, j)

    mark("p10b_turn")

    mark("p11_zsend")
    for i, dz in enumerate(REACH):
        for way in range(2):
            moves[2 * i + way].wait_recv()
        value = image[i] + got[0, i] + got[1, i]
        image[i] = value
        if dz:
            peer = along[(dz - 1) % nz_dev]
            copy = remote(image.at[i], arrived.at[i], last_send.at[i], last_recv.at[i], peer)
            copy.start()
            finals.append((copy, i))
    mark("p12_zwait")
    result = image[REACH.index(0)]
    for copy, slot in finals:
        copy.wait_recv()
        result = result + arrived[slot]
    out[...] = result

    mark("p13_tail")
    for copy, _ in finals:
        copy.wait_send()
    for copy in raws + moves:
        copy.wait_send()

    pltpu.make_async_copy(others, others, small_send.at[0]).wait()

    @pl.when(core == 1)
    def _():
        pltpu.make_async_copy(rest, rest, small_send.at[1]).wait()
        pltpu.make_async_copy(rest, rest, small_send.at[1]).wait()


    @pl.when(depth < nd_dev - 1)
    def _():
        up.wait_send()

    @pl.when(depth > 0)
    def _():
        down.wait_send()

    mark(None)


def solution(mesh):
    nd_dev = mesh.shape["depth"]
    ny_dev = ROWS_Y
    nz_dev = mesh.shape["shot"] // ny_dev

    def on_device(correlation, illumination, aperture):
        shots, nx, ny, nz = correlation.shape
        per_z = nx // ny_dev // nz_dev
        assert per_z == 2 and nz == 128 and nx == 64 and nz_dev == 8
        dma = pltpu.SemaphoreType.DMA
        field = (ny, nz)
        chunks = len(REACH)
        return pl.pallas_call(
            functools.partial(kernel, ny_dev, nz_dev, nd_dev),
            out_shape=jax.ShapeDtypeStruct((per_z, ny, nz), F32),
            in_specs=[pl.BlockSpec(memory_space=pl.ANY)] * 3,
            out_specs=pl.BlockSpec(memory_space=pltpu.VMEM),
            scratch_shapes=[
                pltpu.SMEM((shots, 4), jnp.int32),
                pltpu.VMEM((shots, nx, *field), F32),
                pltpu.VMEM((shots, nx, *field), F32),
                pltpu.VMEM((shots, nx + 2, ny + 2 * PAD, nz), F32),
                pltpu.VMEM((shots, nx, *field), F32),
                pltpu.VMEM((shots, *field), F32),
                pltpu.VMEM(field, F32),
                pltpu.VMEM(field, F32),
                pltpu.VMEM((shots, 2, *field), F32),
                pltpu.VMEM((shots, 2, *field), F32),
                pltpu.VMEM((shots, 2, *field), F32),
                pltpu.VMEM((2, *field), F32),
                pltpu.VMEM((ny_dev * nd_dev, shots, nz), F32),
                pltpu.VMEM((nz_dev, ny_dev * shots, nz), F32),
                pltpu.VMEM((2, shots, chunks, *field), F32),
                pltpu.VMEM((2, shots, chunks, *field), F32),
                pltpu.VMEM((2, shots, 3, *field), F32),
                pltpu.VMEM((2, shots, 3, *field), F32),
                pltpu.VMEM((2, 2, shots, 2, *field), F32),
                pltpu.VMEM((2, 2, shots, 2, *field), F32),
                pltpu.VMEM((4, 2, shots, *field), F32),
                pltpu.VMEM((4, 2, shots, *field), F32),
                pltpu.VMEM((2, per_z, *field), F32),
                pltpu.VMEM((2, chunks, per_z, *field), F32),
                pltpu.VMEM((2, chunks, per_z, *field), F32),
                pltpu.VMEM((chunks, per_z, *field), F32),
                pltpu.VMEM((chunks + 2, per_z, *field), F32),
                dma, dma((shots, PIECES, 2)),
                dma((2,)), dma((2,)), dma((2,)), dma((2,)),
                dma((10,)), dma((10,)), dma((2, chunks)), dma((2, chunks)),
                dma((chunks + 2,)), dma((chunks + 2,)),
            ],
            compiler_params=pltpu.CompilerParams(
                collective_id=0, has_side_effects=True, vmem_limit_bytes=32 << 20
            ),
        )(*(pltpu.with_memory_space_constraint(a, pltpu.HBM) for a in (aperture, correlation, illumination)))

    return jax.shard_map(
        on_device,
        mesh=mesh,
        in_specs=(P("shot", None, None, "depth"), P("shot", None, None, "depth"), P("shot", None)),
        out_specs=P("shot", None, "depth"),
        check_vma=False,
    )
```

```python
import functools

import jax
import jax.numpy as jnp
from jax import lax
from jax.experimental import pallas as pl
from jax.experimental.pallas import tpu as pltpu
from jax.sharding import PartitionSpec as P

ROWS_Y = 4
PIECES = 4
NORM_ROWS = 16
FILTER_ROWS = 16
PAD = 8
REACH = (-3, 3, 1, -1, 0)
EARLY = ((0, 3), (0, -3))
F32 = jnp.float32
MESH = pl.DeviceIdType.MESH


class Marks:
    def __init__(self):
        self.scope = None

    def __call__(self, name):
        if self.scope is not None:
            self.scope.__exit__(None, None, None)
            self.scope = None
        if name:
            self.scope = jax.named_scope(name)
            self.scope.__enter__()


def kernel(
    ny_dev, nz_dev, nd_dev,
    box_hbm, corr, illum, out,
    box, corr_v, illum_v, norm, filt, edge, edge_low, edge_high, rim_v, wrap_v, side_v, mixed,
    energy, peaks, raw_out, raw_in, cross_out, cross_in, beside_out, beside_in, corner_out, corner_in, early_out, early_in, direct, sent, got, image, arrived,
    box_sem, load_sem, edge_send, edge_recv, small_send, small_recv,
    raw_send, raw_recv, move_send, move_recv, last_send, last_recv,
):
    shots, nx, ny, nz = filt.shape
    mark = Marks()
    mark("p00_load_signal")
    shot, depth = lax.axis_index("shot"), lax.axis_index("depth")
    y, z = shot // nz_dev, shot % nz_dev
    per_y = nx // ny_dev
    group = nz // 4
    groups = nx // group

    box_load = pltpu.make_async_copy(box_hbm, box, box_sem)
    box_load.start()
    step = nx // PIECES
    loads = []
    for c in range(PIECES):
        piece = []
        for s in range(shots):
            rows = pl.ds(c * step, step)
            piece.append(pltpu.make_async_copy(corr.at[s, rows], corr_v.at[s, rows], load_sem.at[s, c, 0]))
            piece.append(pltpu.make_async_copy(illum.at[s, rows], illum_v.at[s, rows], load_sem.at[s, c, 1]))
        loads.append(piece)
    for copy in loads[0]:
        copy.start()

    near = []
    for dy in range(ny_dev):
        for dd in range(nd_dev):
            if dy or dd:
                near.append({
                    "shot": lax.rem(y + dy, ny_dev) * nz_dev + z,
                    "depth": lax.rem(depth + dd, nd_dev),
                })
    along = [
        {"shot": y * nz_dev + lax.rem(z + dz, nz_dev), "depth": depth} for dz in range(1, nz_dev)
    ]
    after, before, across = (lax.rem(y + d, ny_dev) for d in (1, ny_dev - 1, ny_dev // 2))
    corners = [
        {"shot": side * nz_dev + lax.rem(z + d, nz_dev), "depth": depth}
        for d in (1, nz_dev - 1)
        for side in (after, before)
    ]
    barrier = pltpu.get_barrier_semaphore()
    core = lax.rem(depth, 2)
    cross_core = [{"shot": peer["shot"], "depth": depth + 1 - 2 * core} for peer in along]

    def hops(count, d):
        return min(d, count - d)

    far = [hops(ny_dev, (i + 1) // nd_dev) + hops(nd_dev, (i + 1) % nd_dev) / 2 for i in range(len(near))]
    far += [hops(nz_dev, i + 1) for i in range(len(along))] * 2 + [2] * len(corners)
    greeted = near + along + cross_core + corners
    for i in sorted(range(len(greeted)), key=lambda i: -far[i]):
        peer = greeted[i]
        pl.semaphore_signal(barrier, inc=1, device_id=peer, device_id_type=MESH)
    for piece in loads[1:]:
        for copy in piece:
            copy.start()

    lane = lax.broadcasted_iota(jnp.int32, (ny, nz), 1)
    row = lax.broadcasted_iota(jnp.int32, (ny, nz), 0)
    ends = (lane == 0) | (lane == nz - 1)
    top, bottom = row == 0, row == ny - 1
    column = lane // 4
    place = lax.rem(lane, 4)
    zero = jnp.zeros((ny, nz), F32)

    def beside_rows(here):
        return jnp.where(top, 0.0, pltpu.roll(here, 1, 0)) + jnp.where(bottom, 0.0, pltpu.roll(here, ny - 1, 0))

    strips = [((row >= box[s, 2]) & (row < box[s, 3])).astype(F32) for s in range(shots)]
    bounds = [(box[s, 0], box[s, 1]) for s in range(shots)]
    blank = jnp.zeros((PAD, nz), F32)

    def clear(x, carry):
        for s in range(shots):
            norm[s, x, :PAD] = blank
            norm[s, x, PAD + ny :] = blank
        return carry

    lax.fori_loop(1, nx + 1, clear, 0)
    for s in range(shots):
        for x in (0, nx + 1):
            norm[s, x] = jnp.zeros((ny + 2 * PAD, nz), F32)
    box_load.wait()
    strips = [((row >= box[s, 2]) & (row < box[s, 3])).astype(F32) for s in range(shots)]
    bounds = [(box[s, 0], box[s, 1]) for s in range(shots)]

    def normalize(k, packs):
        packs = list(packs)
        for s in range(shots):
            for j in range(NORM_ROWS):
                x = k * NORM_ROWS + j
                inside = jnp.where((x >= bounds[s][0]) & (x < bounds[s][1]), 1.0, 0.0).astype(F32)
                value = (strips[s] * inside) * corr_v[s, x] / (illum_v[s, x] + 0.1)
                norm[s, x + 1, PAD : PAD + ny] = value
                turned = pltpu.roll(value, lax.rem(4 * x + 2, nz), 1)
                packs[s] = jnp.where(column == lax.rem(x, group), turned, packs[s])
        return tuple(packs)

    def filter_block(k, sums):
        sums = list(sums)
        for s in range(shots):
            base = k * FILTER_ROWS
            rows = [norm[s, base + i, PAD : PAD + ny] for i in range(FILTER_ROWS + 2)]
            for j in range(FILTER_ROWS):
                here = rows[j + 1]
                beside = rows[j] + rows[j + 2] + (norm[s, base + j + 1, pl.ds(PAD - 1 + lax.min(k, 0), ny)] + norm[s, base + j + 1, pl.ds(PAD + 1 + lax.min(k, 0), ny)])
                beside = beside + pltpu.roll(here, 1, 1) + pltpu.roll(here, nz - 1, 1)
                value = 6.0 * here - beside
                filt[s, base + j] = value
                sums[s] = sums[s] + value * value
        return tuple(sums)

    packs, packed = (zero,) * shots, []
    for c in range(PIECES):
        mark(f"p01_w{c}")
        for copy in loads[c]:
            copy.wait()
        mark(f"p01_x{c}")
        blocks = step // NORM_ROWS
        packs = lax.fori_loop(c * blocks, (c + 1) * blocks, normalize, packs)
        if (c + 1) * step % group == 0:
            packed.append(packs)
            packs = (zero,) * shots

    mark("p02_pack")
    inner = (place == 1) | (place == 2)
    rims = [jnp.where(inner, packed[0][s], pltpu.roll(packed[1][s], 2, 1)) for s in range(shots)]
    odd = lax.rem(lane, 2) == 1
    edge[0] = jnp.where(odd, rims[0], pltpu.roll(rims[1], 1, 1))
    edge[1] = jnp.where(odd, pltpu.roll(rims[1], nz - 1, 1), rims[0])

    mark("p02b_barrier")
    pl.semaphore_wait(barrier, len(near) + len(along) + len(cross_core) + len(corners))
    mark("p03_halo")

    def remote(src, dst, send, recv, peer):
        return pltpu.make_async_remote_copy(
            src_ref=src, dst_ref=dst, send_sem=send, recv_sem=recv, device_id=peer, device_id_type=MESH
        )

    up = remote(edge.at[0], edge_low, edge_send.at[0], edge_recv.at[0], {"shot": shot, "depth": lax.rem(depth + 1, nd_dev)})
    down = remote(edge.at[1], edge_high, edge_send.at[1], edge_recv.at[1], {"shot": shot, "depth": lax.rem(depth + nd_dev - 1, nd_dev)})

    @pl.when(depth < nd_dev - 1)
    def _():
        up.start()

    @pl.when(depth > 0)
    def _():
        down.start()

    @pl.when(depth == 0)
    def _():
        edge_low[...] = jnp.zeros_like(edge_low)

    @pl.when(depth == nd_dev - 1)
    def _():
        edge_high[...] = jnp.zeros_like(edge_high)

    mark("p03_filter")
    sums = lax.fori_loop(0, nx // FILTER_ROWS, filter_block, (zero,) * shots)

    mark("p03a_rim")
    for s in range(shots):
        parts = [packed[g][s] for g in range(groups)]
        backs = [pltpu.roll(part, 4, 1) for part in parts]
        aheads = [pltpu.roll(part, nz - 4, 1) for part in parts]
        for g, part in enumerate(parts):
            back = jnp.where(lane < 4, backs[g - 1] if g else 0.0, backs[g])
            ahead = jnp.where(lane >= nz - 4, aheads[g + 1] if g < groups - 1 else 0.0, aheads[g])
            lower, higher = pltpu.roll(part, 1, 1), pltpu.roll(part, nz - 1, 1)
            deep = jnp.where(place == 1, lower, higher)
            rim_v[s, g] = 6.0 * part - (back + ahead + beside_rows(part) + deep)
            wrap_v[s, g] = jnp.where(place == 1, higher, lower)

    mark("p03w_halo")
    @pl.when(depth > 0)
    def _():
        up.wait_recv()

    @pl.when(depth < nd_dev - 1)
    def _():
        down.wait_recv()

    mark("p04_energy")
    for s in range(shots):
        total = jnp.where(ends, 0.0, sums[s])
        high, low = edge_high[...], edge_low[...]
        for g in range(groups):
            side = jnp.where(
                place == 1,
                pltpu.roll(high, (nz - 1 - 2 * g + s) % nz, 1),
                pltpu.roll(low, (nz + 1 - 2 * g - s) % nz, 1),
            )
            side_v[s, g] = side - wrap_v[s, g]
            rim = rim_v[s, g] - side
            total = total + jnp.where(inner, rim * rim, 0.0)
        energy[0, s : s + 1] = jnp.sum(total, axis=0, keepdims=True)

    def span(i):
        dy, dd = (i + 1) // nd_dev, (i + 1) % nd_dev
        return min(dy, ny_dev - dy) + min(dd, nd_dev - dd) / 2

    for i in sorted(range(len(near)), key=span, reverse=True):
        dy, dd = (i + 1) // nd_dev, (i + 1) % nd_dev
        peer = near[i]
        slot = ((ny_dev - dy) % ny_dev) * nd_dev + (nd_dev - dd) % nd_dev
        remote(energy.at[0], energy.at[slot], small_send.at[0], small_recv.at[0], peer).start()

    mark("p05_raw")
    next_y = {"shot": after * nz_dev + z, "depth": depth}
    prev_y = {"shot": before * nz_dev + z, "depth": depth}
    next_z, prev_z = along[0], along[-1]
    owners = [lax.rem(z + nz_dev + dz, nz_dev) for dz in REACH]
    opposite = lax.rem(z + nz_dev // 2, nz_dev)
    seconds = [lax.rem(z + 2, nz_dev), lax.rem(z + nz_dev - 2, nz_dev)]

    def ends_of(packed_side, x):
        return jnp.where(ends, pltpu.roll(packed_side, lax.rem(2 * nz - 2 - 4 * lax.rem(x, group), nz), 1), 0.0)

    def raw(s, x):
        return filt[s, x] - ends_of(side_v[s, x // group], x)

    chips = (y, after, before)
    raws = []

    def push(out_ref, in_ref, index, peer):
        copy = remote(out_ref, in_ref, raw_send.at[index], raw_recv.at[index], peer)
        copy.start()
        raws.append(copy)

    for way in range(2):
        for s in range(shots):
            for i, chip in enumerate(chips):
                cross_out[way, s, i] = raw(s, chip * per_y + 2 * opposite + way)
    for way in range(2):
        push(cross_out.at[way], cross_in.at[way], way, (next_z, prev_z)[way])
    for way in range(2):
        for s in range(shots):
            for i, owner in enumerate(owners):
                raw_out[way, s, i] = raw(s, across * per_y + 2 * owner + way)
    for way in range(2):
        push(raw_out.at[way], raw_in.at[way], 2 + way, (next_y, prev_y)[way])
    for way in range(2):
        for j in range(2):
            for s in range(shots):
                for i, chip in enumerate(chips[1:]):
                    beside_out[way, j, s, i] = raw(s, chip * per_y + 2 * seconds[way] + j)
    for way in range(2):
        for j in range(2):
            for s in range(shots):
                corner_out[2 * way + j, 0, s] = raw(s, across * per_y + 2 * seconds[way] + j)
                if j == way:
                    corner_out[2 * way + j, 1, s] = raw(s, across * per_y + 2 * opposite + j)
    for k in range(4):
        part = pl.ds(0, 2 if k in (0, 3) else 1)
        push(corner_out.at[k, part], corner_in.at[k, part], 6 + k, corners[k])
    earlies = []
    for way in range(2):
        for n, dz in enumerate(EARLY[way]):
            for s in range(shots):
                early_out[way, n, s] = raw(s, chips[1 + way] * per_y + 2 * owners[REACH.index(dz)] + 1 - way)
        copy = remote(early_out.at[way], early_in.at[way], raw_send.at[10 + way], raw_recv.at[10 + way], (next_y, prev_y)[way])
        copy.start()
        earlies.append(copy)

    mark("p06_wait_energy")
    others = energy.at[pl.ds(1, len(near))]
    pltpu.make_async_copy(others, others, small_recv.at[0]).wait()
    mark("p07_means")
    cells = nx * ny * nz * nd_dev
    means = []
    for dy in range(ny_dev):
        both = jnp.sum(energy[dy * nd_dev : (dy + 1) * nd_dev], axis=0)
        means.append(jnp.broadcast_to(jnp.sum(both, axis=1, keepdims=True) / cells, (shots, nz)))
    for dy in range(ny_dev):
        peaks[0, dy * shots : (dy + 1) * shots] = means[dy]

    @pl.when(core == 1)
    def _():
        for peers in (cross_core, along):
            for i, peer in enumerate(peers):
                remote(peaks.at[0], peaks.at[nz_dev - 1 - i], small_send.at[1], small_recv.at[1], peer).start()

    for way in range(2):
        push(beside_out.at[way], beside_in.at[way], 4 + way, (next_z, prev_z)[way])
    rest = peaks.at[pl.ds(1, len(along))]
    mark("p08_wait_peak")
    pltpu.make_async_copy(rest, rest, small_recv.at[1]).wait()
    mark("p09_weights")
    peak = jnp.max(jnp.max(peaks[...], axis=0), axis=0, keepdims=True)
    scale = 1.0 / float(shots * ny_dev * nz_dev) ** 0.5
    weights = {dz: scale / jnp.sqrt(peaks[dz] + 0.5 * peak + 1.0) for dz in (0, 1, nz_dev - 1)}

    def weight(dy, dz, s):
        return jnp.broadcast_to(weights[dz][dy * shots + s : dy * shots + s + 1], (ny, nz))

    def blend(dy, dz, value):
        return sum(weight(dy, dz, s) * value(s) for s in range(shots))

    for g in range(groups):
        mixed[g] = blend(0, 0, lambda s: side_v[s, g])

    mark("p10_ysend")
    for copy in raws[:8]:
        copy.wait_recv()

    low, high = nz_dev - 1, 1
    behind, ahead = ny_dev - 1, 1

    def share(i, chip, j):
        x = chips[chip] * per_y + 2 * owners[i] + j
        total = blend(0, 0, lambda s: filt[s, x]) - ends_of(mixed[x // group], x)
        onward = chip and j == chip - 1
        side = (behind, ahead)[j]
        if onward:
            total = total + blend(side, 0, lambda s: raw_in[j, s, i])
        if not chip and REACH[i] in EARLY[1 - j]:
            n = EARLY[1 - j].index(REACH[i])
            total = total + blend((behind, ahead)[1 - j], 0, lambda s: early_in[1 - j, n, s])
        if REACH[i] == (3, -3)[j]:
            total = total + blend(0, (low, high)[j], lambda s: cross_in[j, s, chip])
            if onward:
                total = total + blend(side, (low, high)[j], lambda s: corner_in[3 * j, 1, s])
        if REACH[i] in (1, -1):
            way = (1, -1).index(REACH[i])
            if chip:
                total = total + blend(0, (low, high)[way], lambda s: beside_in[way, j, s, chip - 1])
            if onward:
                total = total + blend(side, (low, high)[way], lambda s: corner_in[2 * way + j, 0, s])
        return total

    def rows_of(way, i):
        return (way,) if REACH[i] in EARLY[way] else (0, 1)

    moves, finals = [], []
    for i in range(len(owners)):
        if i == 2:
            for way in range(2):
                for j in range(2):
                    x = y * per_y + 2 * seconds[way] + j
                    direct[way, j] = blend(0, 0, lambda s: filt[s, x]) - ends_of(mixed[x // group], x)
                slot = len(REACH) + way
                copy = remote(direct.at[way], arrived.at[slot], last_send.at[slot], last_recv.at[slot], along[(1, nz_dev - 3)[way]])
                copy.start()
                finals.append((copy, slot))
            for copy in raws[8:]:
                copy.wait_recv()
        for way, peer in enumerate((next_y, prev_y)):
            for j in rows_of(way, i):
                sent[way, i, j] = share(i, 1 + way, j)
            part = pl.ds(rows_of(way, i)[0], len(rows_of(way, i)))
            copy = remote(sent.at[way, i, part], got.at[way, i, part], move_send.at[way, i], move_recv.at[way, i], peer)
            moves.append(copy)
            copy.start()
    for copy in earlies:
        copy.wait_recv()
    for i in range(len(owners)):
        for j in range(2):
            image[i, j] = share(i, 0, j)

    mark("p10b_turn")

    mark("p11_zsend")
    for i, dz in enumerate(REACH):
        for way in range(2):
            moves[2 * i + way].wait_recv()
        for j in range(2):
            value = image[i, j]
            for way in range(2):
                if j in rows_of(way, i):
                    value = value + got[way, i, j]
            image[i, j] = value
        if dz:
            peer = along[(dz - 1) % nz_dev]
            copy = remote(image.at[i], arrived.at[i], last_send.at[i], last_recv.at[i], peer)
            copy.start()
            finals.append((copy, i))
    mark("p12_zwait")
    result = image[REACH.index(0)]
    for copy, slot in finals:
        copy.wait_recv()
        result = result + arrived[slot]
    out[...] = result

    mark("p13_tail")
    for copy, _ in finals:
        copy.wait_send()
    for copy in raws + earlies + moves:
        copy.wait_send()

    pltpu.make_async_copy(others, others, small_send.at[0]).wait()

    @pl.when(core == 1)
    def _():
        pltpu.make_async_copy(rest, rest, small_send.at[1]).wait()
        pltpu.make_async_copy(rest, rest, small_send.at[1]).wait()


    @pl.when(depth < nd_dev - 1)
    def _():
        up.wait_send()

    @pl.when(depth > 0)
    def _():
        down.wait_send()

    mark(None)


def solution(mesh):
    nd_dev = mesh.shape["depth"]
    ny_dev = ROWS_Y
    nz_dev = mesh.shape["shot"] // ny_dev

    def on_device(correlation, illumination, aperture):
        shots, nx, ny, nz = correlation.shape
        per_z = nx // ny_dev // nz_dev
        assert per_z == 2 and nz == 128 and nx == 64 and nz_dev == 8
        dma = pltpu.SemaphoreType.DMA
        field = (ny, nz)
        chunks = len(REACH)
        return pl.pallas_call(
            functools.partial(kernel, ny_dev, nz_dev, nd_dev),
            out_shape=jax.ShapeDtypeStruct((per_z, ny, nz), F32),
            in_specs=[pl.BlockSpec(memory_space=pl.ANY)] * 3,
            out_specs=pl.BlockSpec(memory_space=pltpu.VMEM),
            scratch_shapes=[
                pltpu.SMEM((shots, 4), jnp.int32),
                pltpu.VMEM((shots, nx, *field), F32),
                pltpu.VMEM((shots, nx, *field), F32),
                pltpu.VMEM((shots, nx + 2, ny + 2 * PAD, nz), F32),
                pltpu.VMEM((shots, nx, *field), F32),
                pltpu.VMEM((shots, *field), F32),
                pltpu.VMEM(field, F32),
                pltpu.VMEM(field, F32),
                pltpu.VMEM((shots, 2, *field), F32),
                pltpu.VMEM((shots, 2, *field), F32),
                pltpu.VMEM((shots, 2, *field), F32),
                pltpu.VMEM((2, *field), F32),
                pltpu.VMEM((ny_dev * nd_dev, shots, nz), F32),
                pltpu.VMEM((nz_dev, ny_dev * shots, nz), F32),
                pltpu.VMEM((2, shots, chunks, *field), F32),
                pltpu.VMEM((2, shots, chunks, *field), F32),
                pltpu.VMEM((2, shots, 3, *field), F32),
                pltpu.VMEM((2, shots, 3, *field), F32),
                pltpu.VMEM((2, 2, shots, 2, *field), F32),
                pltpu.VMEM((2, 2, shots, 2, *field), F32),
                pltpu.VMEM((4, 2, shots, *field), F32),
                pltpu.VMEM((4, 2, shots, *field), F32),
                pltpu.VMEM((2, 2, shots, *field), F32),
                pltpu.VMEM((2, 2, shots, *field), F32),
                pltpu.VMEM((2, per_z, *field), F32),
                pltpu.VMEM((2, chunks, per_z, *field), F32),
                pltpu.VMEM((2, chunks, per_z, *field), F32),
                pltpu.VMEM((chunks, per_z, *field), F32),
                pltpu.VMEM((chunks + 2, per_z, *field), F32),
                dma, dma((shots, PIECES, 2)),
                dma((2,)), dma((2,)), dma((2,)), dma((2,)),
                dma((12,)), dma((12,)), dma((2, chunks)), dma((2, chunks)),
                dma((chunks + 2,)), dma((chunks + 2,)),
            ],
            compiler_params=pltpu.CompilerParams(
                collective_id=0, has_side_effects=True, vmem_limit_bytes=32 << 20
            ),
        )(*(pltpu.with_memory_space_constraint(a, pltpu.HBM) for a in (aperture, correlation, illumination)))

    return jax.shard_map(
        on_device,
        mesh=mesh,
        in_specs=(P("shot", None, None, "depth"), P("shot", None, None, "depth"), P("shot", None)),
        out_specs=P("shot", None, "depth"),
        check_vma=False,
    )
```

```python
import functools

import jax
import jax.numpy as jnp
from jax import lax
from jax.experimental import pallas as pl
from jax.experimental.pallas import tpu as pltpu
from jax.sharding import PartitionSpec as P

ROWS_Y = 4
PIECES = 4
NORM_ROWS = 16
FILTER_ROWS = 16
PAD = 8
REACH = (3, -3, 1, -1, 0)
EARLY = ((0, 3), (0, -3))
F32 = jnp.float32
MESH = pl.DeviceIdType.MESH


class Marks:
    def __init__(self):
        self.scope = None

    def __call__(self, name):
        if self.scope is not None:
            self.scope.__exit__(None, None, None)
            self.scope = None
        if name:
            self.scope = jax.named_scope(name)
            self.scope.__enter__()


def kernel(
    ny_dev, nz_dev, nd_dev,
    box_hbm, corr, illum, out,
    box, corr_v, illum_v, norm, filt, edge, edge_low, edge_high, rim_v, wrap_v, side_v, mixed,
    energy, peaks, raw_out, raw_in, cross_out, cross_in, beside_out, beside_in, corner_out, corner_in, early_out, early_in, direct, sent, got, image, arrived,
    box_sem, load_sem, edge_send, edge_recv, small_send, small_recv,
    raw_send, raw_recv, move_send, move_recv, last_send, last_recv,
):
    shots, nx, ny, nz = filt.shape
    mark = Marks()
    mark("p00_load_signal")
    shot, depth = lax.axis_index("shot"), lax.axis_index("depth")
    y, z = shot // nz_dev, shot % nz_dev
    per_y = nx // ny_dev
    group = nz // 4
    groups = nx // group

    box_load = pltpu.make_async_copy(box_hbm, box, box_sem)
    box_load.start()
    step = nx // PIECES
    loads = []
    for c in range(PIECES):
        piece = []
        for s in range(shots):
            rows = pl.ds(c * step, step)
            piece.append(pltpu.make_async_copy(corr.at[s, rows], corr_v.at[s, rows], load_sem.at[s, c, 0]))
            piece.append(pltpu.make_async_copy(illum.at[s, rows], illum_v.at[s, rows], load_sem.at[s, c, 1]))
        loads.append(piece)
    for copy in loads[0]:
        copy.start()

    near = []
    for dy in range(ny_dev):
        for dd in range(nd_dev):
            if dy or dd:
                near.append({
                    "shot": lax.rem(y + dy, ny_dev) * nz_dev + z,
                    "depth": lax.rem(depth + dd, nd_dev),
                })
    along = [
        {"shot": y * nz_dev + lax.rem(z + dz, nz_dev), "depth": depth} for dz in range(1, nz_dev)
    ]
    after, before, across = (lax.rem(y + d, ny_dev) for d in (1, ny_dev - 1, ny_dev // 2))
    corners = [
        {"shot": side * nz_dev + lax.rem(z + d, nz_dev), "depth": depth}
        for d in (1, nz_dev - 1)
        for side in (after, before)
    ]
    barrier = pltpu.get_barrier_semaphore()
    core = lax.rem(depth, 2)
    cross_core = [{"shot": peer["shot"], "depth": depth + 1 - 2 * core} for peer in along]

    def hops(count, d):
        return min(d, count - d)

    far = [hops(ny_dev, (i + 1) // nd_dev) + hops(nd_dev, (i + 1) % nd_dev) / 2 for i in range(len(near))]
    far += [hops(nz_dev, i + 1) for i in range(len(along))] * 2 + [2] * len(corners)
    greeted = near + along + cross_core + corners
    for i in sorted(range(len(greeted)), key=lambda i: -far[i]):
        peer = greeted[i]
        pl.semaphore_signal(barrier, inc=1, device_id=peer, device_id_type=MESH)
    for piece in loads[1:]:
        for copy in piece:
            copy.start()

    lane = lax.broadcasted_iota(jnp.int32, (ny, nz), 1)
    row = lax.broadcasted_iota(jnp.int32, (ny, nz), 0)
    ends = (lane == 0) | (lane == nz - 1)
    top, bottom = row == 0, row == ny - 1
    column = lane // 4
    place = lax.rem(lane, 4)
    zero = jnp.zeros((ny, nz), F32)

    def beside_rows(here):
        return jnp.where(top, 0.0, pltpu.roll(here, 1, 0)) + jnp.where(bottom, 0.0, pltpu.roll(here, ny - 1, 0))

    strips = [((row >= box[s, 2]) & (row < box[s, 3])).astype(F32) for s in range(shots)]
    bounds = [(box[s, 0], box[s, 1]) for s in range(shots)]
    blank = jnp.zeros((PAD, nz), F32)

    def clear(x, carry):
        for s in range(shots):
            norm[s, x, :PAD] = blank
            norm[s, x, PAD + ny :] = blank
        return carry

    lax.fori_loop(1, nx + 1, clear, 0)
    for s in range(shots):
        for x in (0, nx + 1):
            norm[s, x] = jnp.zeros((ny + 2 * PAD, nz), F32)
    box_load.wait()
    strips = [((row >= box[s, 2]) & (row < box[s, 3])).astype(F32) for s in range(shots)]
    bounds = [(box[s, 0], box[s, 1]) for s in range(shots)]

    def normalize(k, packs):
        packs = list(packs)
        for s in range(shots):
            for j in range(NORM_ROWS):
                x = k * NORM_ROWS + j
                inside = jnp.where((x >= bounds[s][0]) & (x < bounds[s][1]), 1.0, 0.0).astype(F32)
                value = (strips[s] * inside) * corr_v[s, x] / (illum_v[s, x] + 0.1)
                norm[s, x + 1, PAD : PAD + ny] = value
                turned = pltpu.roll(value, lax.rem(4 * x + 2, nz), 1)
                packs[s] = jnp.where(column == lax.rem(x, group), turned, packs[s])
        return tuple(packs)

    def filter_block(k, sums):
        sums = list(sums)
        for s in range(shots):
            base = k * FILTER_ROWS
            rows = [norm[s, base + i, PAD : PAD + ny] for i in range(FILTER_ROWS + 2)]
            for j in range(FILTER_ROWS):
                here = rows[j + 1]
                beside = rows[j] + rows[j + 2] + (norm[s, base + j + 1, pl.ds(PAD - 1 + lax.min(k, 0), ny)] + norm[s, base + j + 1, pl.ds(PAD + 1 + lax.min(k, 0), ny)])
                beside = beside + pltpu.roll(here, 1, 1) + pltpu.roll(here, nz - 1, 1)
                value = 6.0 * here - beside
                filt[s, base + j] = value
                sums[s] = sums[s] + value * value
        return tuple(sums)

    packs, packed = (zero,) * shots, []
    for c in range(PIECES):
        mark(f"p01_w{c}")
        for copy in loads[c]:
            copy.wait()
        mark(f"p01_x{c}")
        blocks = step // NORM_ROWS
        packs = lax.fori_loop(c * blocks, (c + 1) * blocks, normalize, packs)
        if (c + 1) * step % group == 0:
            packed.append(packs)
            packs = (zero,) * shots

    mark("p02_pack")
    inner = (place == 1) | (place == 2)
    rims = [jnp.where(inner, packed[0][s], pltpu.roll(packed[1][s], 2, 1)) for s in range(shots)]
    odd = lax.rem(lane, 2) == 1
    edge[0] = jnp.where(odd, rims[0], pltpu.roll(rims[1], 1, 1))
    edge[1] = jnp.where(odd, pltpu.roll(rims[1], nz - 1, 1), rims[0])

    mark("p02b_barrier")
    pl.semaphore_wait(barrier, len(near) + len(along) + len(cross_core) + len(corners))
    mark("p03_halo")

    def remote(src, dst, send, recv, peer):
        return pltpu.make_async_remote_copy(
            src_ref=src, dst_ref=dst, send_sem=send, recv_sem=recv, device_id=peer, device_id_type=MESH
        )

    up = remote(edge.at[0], edge_low, edge_send.at[0], edge_recv.at[0], {"shot": shot, "depth": lax.rem(depth + 1, nd_dev)})
    down = remote(edge.at[1], edge_high, edge_send.at[1], edge_recv.at[1], {"shot": shot, "depth": lax.rem(depth + nd_dev - 1, nd_dev)})

    @pl.when(depth < nd_dev - 1)
    def _():
        up.start()

    @pl.when(depth > 0)
    def _():
        down.start()

    @pl.when(depth == 0)
    def _():
        edge_low[...] = jnp.zeros_like(edge_low)

    @pl.when(depth == nd_dev - 1)
    def _():
        edge_high[...] = jnp.zeros_like(edge_high)

    mark("p03_filter")
    sums = lax.fori_loop(0, nx // FILTER_ROWS, filter_block, (zero,) * shots)

    mark("p03a_rim")
    for s in range(shots):
        parts = [packed[g][s] for g in range(groups)]
        backs = [pltpu.roll(part, 4, 1) for part in parts]
        aheads = [pltpu.roll(part, nz - 4, 1) for part in parts]
        for g, part in enumerate(parts):
            back = jnp.where(lane < 4, backs[g - 1] if g else 0.0, backs[g])
            ahead = jnp.where(lane >= nz - 4, aheads[g + 1] if g < groups - 1 else 0.0, aheads[g])
            lower, higher = pltpu.roll(part, 1, 1), pltpu.roll(part, nz - 1, 1)
            deep = jnp.where(place == 1, lower, higher)
            rim_v[s, g] = 6.0 * part - (back + ahead + beside_rows(part) + deep)
            wrap_v[s, g] = jnp.where(place == 1, higher, lower)

    mark("p03w_halo")
    @pl.when(depth > 0)
    def _():
        up.wait_recv()

    @pl.when(depth < nd_dev - 1)
    def _():
        down.wait_recv()

    mark("p04_energy")
    for s in range(shots):
        total = jnp.where(ends, 0.0, sums[s])
        high, low = edge_high[...], edge_low[...]
        for g in range(groups):
            side = jnp.where(
                place == 1,
                pltpu.roll(high, (nz - 1 - 2 * g + s) % nz, 1),
                pltpu.roll(low, (nz + 1 - 2 * g - s) % nz, 1),
            )
            side_v[s, g] = side - wrap_v[s, g]
            rim = rim_v[s, g] - side
            total = total + jnp.where(inner, rim * rim, 0.0)
        energy[0, s : s + 1] = jnp.sum(total, axis=0, keepdims=True)

    def span(i):
        dy, dd = (i + 1) // nd_dev, (i + 1) % nd_dev
        return min(dy, ny_dev - dy) + min(dd, nd_dev - dd) / 2

    for i in sorted(range(len(near)), key=span, reverse=True):
        dy, dd = (i + 1) // nd_dev, (i + 1) % nd_dev
        peer = near[i]
        slot = ((ny_dev - dy) % ny_dev) * nd_dev + (nd_dev - dd) % nd_dev
        copy = remote(energy.at[0], energy.at[slot], small_send.at[0], small_recv.at[0], peer)
        pl.when(core == 1 - dd % 2)(copy.start)

    mark("p05_raw")
    next_y = {"shot": after * nz_dev + z, "depth": depth}
    prev_y = {"shot": before * nz_dev + z, "depth": depth}
    next_z, prev_z = along[0], along[-1]
    owners = [lax.rem(z + nz_dev + dz, nz_dev) for dz in REACH]
    opposite = lax.rem(z + nz_dev // 2, nz_dev)
    seconds = [lax.rem(z + 2, nz_dev), lax.rem(z + nz_dev - 2, nz_dev)]

    def ends_of(packed_side, x):
        return jnp.where(ends, pltpu.roll(packed_side, lax.rem(2 * nz - 2 - 4 * lax.rem(x, group), nz), 1), 0.0)

    def raw(s, x):
        return filt[s, x] - ends_of(side_v[s, x // group], x)

    chips = (y, after, before)
    raws = []

    def push(out_ref, in_ref, index, peer):
        copy = remote(out_ref, in_ref, raw_send.at[index], raw_recv.at[index], peer)
        copy.start()
        raws.append(copy)

    for way in range(2):
        for s in range(shots):
            for i, chip in enumerate(chips):
                cross_out[way, s, i] = raw(s, chip * per_y + 2 * opposite + way)
    for way in range(2):
        push(cross_out.at[way], cross_in.at[way], way, (next_z, prev_z)[way])
    for way in range(2):
        for s in range(shots):
            for i, owner in enumerate(owners):
                raw_out[way, s, i] = raw(s, across * per_y + 2 * owner + way)
    for way in range(2):
        push(raw_out.at[way], raw_in.at[way], 2 + way, (next_y, prev_y)[way])
    for way in range(2):
        for j in range(2):
            for s in range(shots):
                for i, chip in enumerate(chips[1:]):
                    beside_out[way, j, s, i] = raw(s, chip * per_y + 2 * seconds[way] + j)
    for way in range(2):
        for j in range(2):
            for s in range(shots):
                corner_out[2 * way + j, 0, s] = raw(s, across * per_y + 2 * seconds[way] + j)
                if j == way:
                    corner_out[2 * way + j, 1, s] = raw(s, across * per_y + 2 * opposite + j)
    for k in range(4):
        part = pl.ds(0, 2 if k in (0, 3) else 1)
        push(corner_out.at[k, part], corner_in.at[k, part], 6 + k, corners[k])
    earlies = []
    for way in range(2):
        for n, dz in enumerate(EARLY[way]):
            for s in range(shots):
                early_out[way, n, s] = raw(s, chips[1 + way] * per_y + 2 * owners[REACH.index(dz)] + 1 - way)
        copy = remote(early_out.at[way], early_in.at[way], raw_send.at[10 + way], raw_recv.at[10 + way], (next_y, prev_y)[way])
        copy.start()
        earlies.append(copy)

    mark("p06_wait_energy")
    others = energy.at[pl.ds(1, len(near))]
    cells = nx * ny * nz * nd_dev

    def told(src, dst, peer, recv):
        return remote(peaks.at[src], peaks.at[dst], small_send.at[1], small_recv.at[recv], peer)

    @pl.when(core == 1)
    def _():
        pltpu.make_async_copy(others, others, small_recv.at[0]).wait()
        for dy in range(ny_dev):
            both = jnp.sum(energy[dy * nd_dev : (dy + 1) * nd_dev], axis=0)
            mean = jnp.sum(both, axis=1, keepdims=True) / cells
            peaks[0, dy * shots : (dy + 1) * shots] = jnp.broadcast_to(mean, (shots, nz))
        for peers in (cross_core, along):
            for i, peer in enumerate(peers):
                told(0, nz_dev - 1 - i, peer, 1).start()
        told(0, 0, {"shot": shot, "depth": depth - 1}, 2).start()

    @pl.when(core == 0)
    def _():
        pltpu.make_async_copy(peaks.at[0], peaks.at[0], small_recv.at[2]).wait()

    for way in range(2):
        push(beside_out.at[way], beside_in.at[way], 4 + way, (next_z, prev_z)[way])
    rest = peaks.at[pl.ds(1, len(along))]
    mark("p08_wait_peak")
    pltpu.make_async_copy(rest, rest, small_recv.at[1]).wait()
    mark("p09_weights")
    peak = jnp.max(jnp.max(peaks[...], axis=0), axis=0, keepdims=True)
    scale = 1.0 / float(shots * ny_dev * nz_dev) ** 0.5
    weights = {dz: scale / jnp.sqrt(peaks[dz] + 0.5 * peak + 1.0) for dz in (0, 1, nz_dev - 1)}

    def weight(dy, dz, s):
        return jnp.broadcast_to(weights[dz][dy * shots + s : dy * shots + s + 1], (ny, nz))

    def blend(dy, dz, value):
        return sum(weight(dy, dz, s) * value(s) for s in range(shots))

    for g in range(groups):
        mixed[g] = blend(0, 0, lambda s: side_v[s, g])

    mark("p10_ysend")
    for copy in raws[:8]:
        copy.wait_recv()

    low, high = nz_dev - 1, 1
    behind, ahead = ny_dev - 1, 1

    def share(i, chip, j):
        x = chips[chip] * per_y + 2 * owners[i] + j
        total = blend(0, 0, lambda s: filt[s, x]) - ends_of(mixed[x // group], x)
        onward = chip and j == chip - 1
        side = (behind, ahead)[j]
        if onward:
            total = total + blend(side, 0, lambda s: raw_in[j, s, i])
        if not chip and REACH[i] in EARLY[1 - j]:
            n = EARLY[1 - j].index(REACH[i])
            total = total + blend((behind, ahead)[1 - j], 0, lambda s: early_in[1 - j, n, s])
        if REACH[i] == (3, -3)[j]:
            total = total + blend(0, (low, high)[j], lambda s: cross_in[j, s, chip])
            if onward:
                total = total + blend(side, (low, high)[j], lambda s: corner_in[3 * j, 1, s])
        if REACH[i] in (1, -1):
            way = (1, -1).index(REACH[i])
            if chip:
                total = total + blend(0, (low, high)[way], lambda s: beside_in[way, j, s, chip - 1])
            if onward:
                total = total + blend(side, (low, high)[way], lambda s: corner_in[2 * way + j, 0, s])
        return total

    def rows_of(way, i):
        return (way,) if REACH[i] in EARLY[way] else (0, 1)

    moves, finals = [], []
    for i in range(len(owners)):
        if i == 2:
            for way in range(2):
                for j in range(2):
                    x = y * per_y + 2 * seconds[way] + j
                    direct[way, j] = blend(0, 0, lambda s: filt[s, x]) - ends_of(mixed[x // group], x)
                slot = len(REACH) + way
                copy = remote(direct.at[way], arrived.at[slot], last_send.at[slot], last_recv.at[slot], along[(1, nz_dev - 3)[way]])
                copy.start()
                finals.append((copy, slot))
            for copy in raws[8:]:
                copy.wait_recv()
        for way, peer in enumerate((next_y, prev_y)):
            for j in rows_of(way, i):
                sent[way, i, j] = share(i, 1 + way, j)
            part = pl.ds(rows_of(way, i)[0], len(rows_of(way, i)))
            copy = remote(sent.at[way, i, part], got.at[way, i, part], move_send.at[way, i], move_recv.at[way, i], peer)
            moves.append(copy)
            copy.start()
    for copy in earlies:
        copy.wait_recv()
    for i in range(len(owners)):
        for j in range(2):
            image[i, j] = share(i, 0, j)

    mark("p10b_turn")

    mark("p11_zsend")
    for i, dz in enumerate(REACH):
        for way in range(2):
            moves[2 * i + way].wait_recv()
        for j in range(2):
            value = image[i, j]
            for way in range(2):
                if j in rows_of(way, i):
                    value = value + got[way, i, j]
            image[i, j] = value
        if dz:
            peer = along[(dz - 1) % nz_dev]
            copy = remote(image.at[i], arrived.at[i], last_send.at[i], last_recv.at[i], peer)
            copy.start()
            finals.append((copy, i))
    mark("p12_zwait")
    result = image[REACH.index(0)]
    for copy, slot in finals:
        copy.wait_recv()
        result = result + arrived[slot]
    out[...] = result

    mark("p13_tail")
    for copy, _ in finals:
        copy.wait_send()
    for copy in raws + earlies + moves:
        copy.wait_send()

    for k in range(2):
        part = energy.at[pl.ds(1, len(near) // 2 + 1 - k)]
        pl.when(core == k)(pltpu.make_async_copy(part, part, small_send.at[0]).wait)

    @pl.when(core == 1)
    def _():
        pltpu.make_async_copy(rest, rest, small_send.at[1]).wait()
        pltpu.make_async_copy(peaks, peaks, small_send.at[1]).wait()


    @pl.when(depth < nd_dev - 1)
    def _():
        up.wait_send()

    @pl.when(depth > 0)
    def _():
        down.wait_send()

    mark(None)


def solution(mesh):
    nd_dev = mesh.shape["depth"]
    ny_dev = ROWS_Y
    nz_dev = mesh.shape["shot"] // ny_dev

    def on_device(correlation, illumination, aperture):
        shots, nx, ny, nz = correlation.shape
        per_z = nx // ny_dev // nz_dev
        assert per_z == 2 and nz == 128 and nx == 64 and nz_dev == 8
        dma = pltpu.SemaphoreType.DMA
        field = (ny, nz)
        chunks = len(REACH)
        return pl.pallas_call(
            functools.partial(kernel, ny_dev, nz_dev, nd_dev),
            out_shape=jax.ShapeDtypeStruct((per_z, ny, nz), F32),
            in_specs=[pl.BlockSpec(memory_space=pl.ANY)] * 3,
            out_specs=pl.BlockSpec(memory_space=pltpu.VMEM),
            scratch_shapes=[
                pltpu.SMEM((shots, 4), jnp.int32),
                pltpu.VMEM((shots, nx, *field), F32),
                pltpu.VMEM((shots, nx, *field), F32),
                pltpu.VMEM((shots, nx + 2, ny + 2 * PAD, nz), F32),
                pltpu.VMEM((shots, nx, *field), F32),
                pltpu.VMEM((shots, *field), F32),
                pltpu.VMEM(field, F32),
                pltpu.VMEM(field, F32),
                pltpu.VMEM((shots, 2, *field), F32),
                pltpu.VMEM((shots, 2, *field), F32),
                pltpu.VMEM((shots, 2, *field), F32),
                pltpu.VMEM((2, *field), F32),
                pltpu.VMEM((ny_dev * nd_dev, shots, nz), F32),
                pltpu.VMEM((nz_dev, ny_dev * shots, nz), F32),
                pltpu.VMEM((2, shots, chunks, *field), F32),
                pltpu.VMEM((2, shots, chunks, *field), F32),
                pltpu.VMEM((2, shots, 3, *field), F32),
                pltpu.VMEM((2, shots, 3, *field), F32),
                pltpu.VMEM((2, 2, shots, 2, *field), F32),
                pltpu.VMEM((2, 2, shots, 2, *field), F32),
                pltpu.VMEM((4, 2, shots, *field), F32),
                pltpu.VMEM((4, 2, shots, *field), F32),
                pltpu.VMEM((2, 2, shots, *field), F32),
                pltpu.VMEM((2, 2, shots, *field), F32),
                pltpu.VMEM((2, per_z, *field), F32),
                pltpu.VMEM((2, chunks, per_z, *field), F32),
                pltpu.VMEM((2, chunks, per_z, *field), F32),
                pltpu.VMEM((chunks, per_z, *field), F32),
                pltpu.VMEM((chunks + 2, per_z, *field), F32),
                dma, dma((shots, PIECES, 2)),
                dma((2,)), dma((2,)), dma((2,)), dma((3,)),
                dma((12,)), dma((12,)), dma((2, chunks)), dma((2, chunks)),
                dma((chunks + 2,)), dma((chunks + 2,)),
            ],
            compiler_params=pltpu.CompilerParams(
                collective_id=0, has_side_effects=True, vmem_limit_bytes=32 << 20
            ),
        )(*(pltpu.with_memory_space_constraint(a, pltpu.HBM) for a in (aperture, correlation, illumination)))

    return jax.shard_map(
        on_device,
        mesh=mesh,
        in_specs=(P("shot", None, None, "depth"), P("shot", None, None, "depth"), P("shot", None)),
        out_specs=P("shot", None, "depth"),
        check_vma=False,
    )
```

```python
import functools

import jax
import jax.numpy as jnp
from jax import lax
from jax.experimental import pallas as pl
from jax.experimental.pallas import tpu as pltpu
from jax.sharding import PartitionSpec as P

ROWS_Y = 4
PIECES = 4
NORM_ROWS = 16
FILTER_ROWS = 16
PAD = 8
REACH = (3, -3, 1, -1, 0)
EARLY = ((0, 3), (0, -3))
F32 = jnp.float32
MESH = pl.DeviceIdType.MESH


class Marks:
    def __init__(self):
        self.scope = None

    def __call__(self, name):
        if self.scope is not None:
            self.scope.__exit__(None, None, None)
            self.scope = None
        if name:
            self.scope = jax.named_scope(name)
            self.scope.__enter__()


def kernel(
    ny_dev, nz_dev, nd_dev,
    box_hbm, corr, illum, out,
    box, corr_v, illum_v, norm, filt, edge, edge_low, edge_high, rim_v, wrap_v, side_v, mixed,
    energy, peaks, raw_out, raw_in, cross_out, cross_in, beside_out, beside_in, corner_out, corner_in, early_out, early_in, direct, sent, got, image, arrived,
    box_sem, load_sem, edge_send, edge_recv, small_send, small_recv,
    raw_send, raw_recv, move_send, move_recv, last_send, last_recv,
):
    shots, nx, ny, nz = filt.shape
    mark = Marks()
    mark("p00_load_signal")
    shot, depth = lax.axis_index("shot"), lax.axis_index("depth")
    y, z = shot // nz_dev, shot % nz_dev
    per_y = nx // ny_dev
    group = nz // 4
    groups = nx // group

    box_load = pltpu.make_async_copy(box_hbm, box, box_sem)
    box_load.start()
    step = nx // PIECES
    loads = []
    for c in range(PIECES):
        piece = []
        for s in range(shots):
            rows = pl.ds(c * step, step)
            piece.append(pltpu.make_async_copy(corr.at[s, rows], corr_v.at[s, rows], load_sem.at[s, c, 0]))
            piece.append(pltpu.make_async_copy(illum.at[s, rows], illum_v.at[s, rows], load_sem.at[s, c, 1]))
        loads.append(piece)
    for copy in loads[0]:
        copy.start()

    near = []
    for dy in range(ny_dev):
        for dd in range(nd_dev):
            if dy or dd:
                near.append({
                    "shot": lax.rem(y + dy, ny_dev) * nz_dev + z,
                    "depth": lax.rem(depth + dd, nd_dev),
                })
    along = [
        {"shot": y * nz_dev + lax.rem(z + dz, nz_dev), "depth": depth} for dz in range(1, nz_dev)
    ]
    after, before, across = (lax.rem(y + d, ny_dev) for d in (1, ny_dev - 1, ny_dev // 2))
    corners = [
        {"shot": side * nz_dev + lax.rem(z + d, nz_dev), "depth": depth}
        for d in (1, nz_dev - 1)
        for side in (after, before)
    ]
    barrier = pltpu.get_barrier_semaphore()
    core = lax.rem(depth, 2)
    cross_core = [{"shot": peer["shot"], "depth": depth + 1 - 2 * core} for peer in along]

    def hops(count, d):
        return min(d, count - d)

    far = [hops(ny_dev, (i + 1) // nd_dev) + hops(nd_dev, (i + 1) % nd_dev) / 2 for i in range(len(near))]
    far += [hops(nz_dev, i + 1) for i in range(len(along))] * 2 + [2] * len(corners)
    greeted = near + along + cross_core + corners
    unmet = 0
    for i in sorted(range(len(greeted)), key=lambda i: -far[i]):
        peer = greeted[i]
        dy, dd = (i + 1) // nd_dev, (i + 1) % nd_dev
        apart = i < len(near) and dd % 2 == 0 and not (dd == 0 and 2 * dy != ny_dev)
        unmet += apart

        def greet(peer=peer):
            pl.semaphore_signal(barrier, inc=1, device_id=peer, device_id_type=MESH)

        if apart:
            pl.when(core == 1)(greet)
        else:
            greet()
    for piece in loads[1:]:
        for copy in piece:
            copy.start()

    lane = lax.broadcasted_iota(jnp.int32, (ny, nz), 1)
    row = lax.broadcasted_iota(jnp.int32, (ny, nz), 0)
    ends = (lane == 0) | (lane == nz - 1)
    top, bottom = row == 0, row == ny - 1
    column = lane // 4
    place = lax.rem(lane, 4)
    zero = jnp.zeros((ny, nz), F32)

    def beside_rows(here):
        return jnp.where(top, 0.0, pltpu.roll(here, 1, 0)) + jnp.where(bottom, 0.0, pltpu.roll(here, ny - 1, 0))

    strips = [((row >= box[s, 2]) & (row < box[s, 3])).astype(F32) for s in range(shots)]
    bounds = [(box[s, 0], box[s, 1]) for s in range(shots)]
    blank = jnp.zeros((PAD, nz), F32)

    def clear(x, carry):
        for s in range(shots):
            norm[s, x, :PAD] = blank
            norm[s, x, PAD + ny :] = blank
        return carry

    lax.fori_loop(1, nx + 1, clear, 0)
    for s in range(shots):
        for x in (0, nx + 1):
            norm[s, x] = jnp.zeros((ny + 2 * PAD, nz), F32)
    box_load.wait()
    strips = [((row >= box[s, 2]) & (row < box[s, 3])).astype(F32) for s in range(shots)]
    bounds = [(box[s, 0], box[s, 1]) for s in range(shots)]

    def normalize(k, packs):
        packs = list(packs)
        for s in range(shots):
            for j in range(NORM_ROWS):
                x = k * NORM_ROWS + j
                inside = jnp.where((x >= bounds[s][0]) & (x < bounds[s][1]), 1.0, 0.0).astype(F32)
                value = (strips[s] * inside) * corr_v[s, x] / (illum_v[s, x] + 0.1)
                norm[s, x + 1, PAD : PAD + ny] = value
                turned = pltpu.roll(value, lax.rem(4 * x + 2, nz), 1)
                packs[s] = jnp.where(column == lax.rem(x, group), turned, packs[s])
        return tuple(packs)

    def filter_block(k, sums):
        sums = list(sums)
        for s in range(shots):
            base = k * FILTER_ROWS
            rows = [norm[s, base + i, PAD : PAD + ny] for i in range(FILTER_ROWS + 2)]
            for j in range(FILTER_ROWS):
                here = rows[j + 1]
                beside = rows[j] + rows[j + 2] + (norm[s, base + j + 1, pl.ds(PAD - 1 + lax.min(k, 0), ny)] + norm[s, base + j + 1, pl.ds(PAD + 1 + lax.min(k, 0), ny)])
                beside = beside + pltpu.roll(here, 1, 1) + pltpu.roll(here, nz - 1, 1)
                value = 6.0 * here - beside
                filt[s, base + j] = value
                sums[s] = sums[s] + value * value
        return tuple(sums)

    packs, packed = (zero,) * shots, []
    for c in range(PIECES):
        mark(f"p01_w{c}")
        for copy in loads[c]:
            copy.wait()
        mark(f"p01_x{c}")
        blocks = step // NORM_ROWS
        packs = lax.fori_loop(c * blocks, (c + 1) * blocks, normalize, packs)
        if (c + 1) * step % group == 0:
            packed.append(packs)
            packs = (zero,) * shots

    mark("p02_pack")
    inner = (place == 1) | (place == 2)
    rims = [jnp.where(inner, packed[0][s], pltpu.roll(packed[1][s], 2, 1)) for s in range(shots)]
    odd = lax.rem(lane, 2) == 1
    edge[0] = jnp.where(odd, rims[0], pltpu.roll(rims[1], 1, 1))
    edge[1] = jnp.where(odd, pltpu.roll(rims[1], nz - 1, 1), rims[0])

    mark("p02b_barrier")
    pl.semaphore_wait(barrier, len(greeted) - unmet * (1 - core))
    mark("p03_halo")

    def remote(src, dst, send, recv, peer):
        return pltpu.make_async_remote_copy(
            src_ref=src, dst_ref=dst, send_sem=send, recv_sem=recv, device_id=peer, device_id_type=MESH
        )

    up = remote(edge.at[0], edge_low, edge_send.at[0], edge_recv.at[0], {"shot": shot, "depth": lax.rem(depth + 1, nd_dev)})
    down = remote(edge.at[1], edge_high, edge_send.at[1], edge_recv.at[1], {"shot": shot, "depth": lax.rem(depth + nd_dev - 1, nd_dev)})

    @pl.when(depth < nd_dev - 1)
    def _():
        up.start()

    @pl.when(depth > 0)
    def _():
        down.start()

    @pl.when(depth == 0)
    def _():
        edge_low[...] = jnp.zeros_like(edge_low)

    @pl.when(depth == nd_dev - 1)
    def _():
        edge_high[...] = jnp.zeros_like(edge_high)

    mark("p03_filter")
    sums = lax.fori_loop(0, nx // FILTER_ROWS, filter_block, (zero,) * shots)

    mark("p03a_rim")
    for s in range(shots):
        parts = [packed[g][s] for g in range(groups)]
        backs = [pltpu.roll(part, 4, 1) for part in parts]
        aheads = [pltpu.roll(part, nz - 4, 1) for part in parts]
        for g, part in enumerate(parts):
            back = jnp.where(lane < 4, backs[g - 1] if g else 0.0, backs[g])
            ahead = jnp.where(lane >= nz - 4, aheads[g + 1] if g < groups - 1 else 0.0, aheads[g])
            lower, higher = pltpu.roll(part, 1, 1), pltpu.roll(part, nz - 1, 1)
            deep = jnp.where(place == 1, lower, higher)
            rim_v[s, g] = 6.0 * part - (back + ahead + beside_rows(part) + deep)
            wrap_v[s, g] = jnp.where(place == 1, higher, lower)

    mark("p03w_halo")
    @pl.when(depth > 0)
    def _():
        up.wait_recv()

    @pl.when(depth < nd_dev - 1)
    def _():
        down.wait_recv()

    mark("p04_energy")
    for s in range(shots):
        total = jnp.where(ends, 0.0, sums[s])
        high, low = edge_high[...], edge_low[...]
        for g in range(groups):
            side = jnp.where(
                place == 1,
                pltpu.roll(high, (nz - 1 - 2 * g + s) % nz, 1),
                pltpu.roll(low, (nz + 1 - 2 * g - s) % nz, 1),
            )
            side_v[s, g] = side - wrap_v[s, g]
            rim = rim_v[s, g] - side
            total = total + jnp.where(inner, rim * rim, 0.0)
        energy[0, s : s + 1] = jnp.sum(total, axis=0, keepdims=True)

    def span(i):
        dy, dd = (i + 1) // nd_dev, (i + 1) % nd_dev
        return min(dy, ny_dev - dy) + min(dd, nd_dev - dd) / 2

    for i in sorted(range(len(near)), key=span, reverse=True):
        dy, dd = (i + 1) // nd_dev, (i + 1) % nd_dev
        peer = near[i]
        slot = ((ny_dev - dy) % ny_dev) * nd_dev + (nd_dev - dd) % nd_dev
        copy = remote(energy.at[0], energy.at[slot], small_send.at[0], small_recv.at[0], peer)
        pl.when(core == 1 - dd % 2)(copy.start)

    mark("p05_raw")
    next_y = {"shot": after * nz_dev + z, "depth": depth}
    prev_y = {"shot": before * nz_dev + z, "depth": depth}
    next_z, prev_z = along[0], along[-1]
    owners = [lax.rem(z + nz_dev + dz, nz_dev) for dz in REACH]
    opposite = lax.rem(z + nz_dev // 2, nz_dev)
    seconds = [lax.rem(z + 2, nz_dev), lax.rem(z + nz_dev - 2, nz_dev)]

    def ends_of(packed_side, x):
        return jnp.where(ends, pltpu.roll(packed_side, lax.rem(2 * nz - 2 - 4 * lax.rem(x, group), nz), 1), 0.0)

    def raw(s, x):
        return filt[s, x] - ends_of(side_v[s, x // group], x)

    chips = (y, after, before)
    raws = []

    def push(out_ref, in_ref, index, peer):
        copy = remote(out_ref, in_ref, raw_send.at[index], raw_recv.at[index], peer)
        copy.start()
        raws.append(copy)

    for way in range(2):
        for s in range(shots):
            for i, chip in enumerate(chips):
                cross_out[way, s, i] = raw(s, chip * per_y + 2 * opposite + way)
    for way in range(2):
        push(cross_out.at[way], cross_in.at[way], way, (next_z, prev_z)[way])
    for way in range(2):
        for s in range(shots):
            for i, owner in enumerate(owners):
                raw_out[way, s, i] = raw(s, across * per_y + 2 * owner + way)
    for way in range(2):
        push(raw_out.at[way], raw_in.at[way], 2 + way, (next_y, prev_y)[way])
    for way in range(2):
        for j in range(2):
            for s in range(shots):
                for i, chip in enumerate(chips[1:]):
                    beside_out[way, j, s, i] = raw(s, chip * per_y + 2 * seconds[way] + j)
    for way in range(2):
        for j in range(2):
            for s in range(shots):
                corner_out[2 * way + j, 0, s] = raw(s, across * per_y + 2 * seconds[way] + j)
                if j == way:
                    corner_out[2 * way + j, 1, s] = raw(s, across * per_y + 2 * opposite + j)
    for k in range(4):
        part = pl.ds(0, 2 if k in (0, 3) else 1)
        push(corner_out.at[k, part], corner_in.at[k, part], 6 + k, corners[k])
    earlies = []
    for way in range(2):
        for n, dz in enumerate(EARLY[way]):
            for s in range(shots):
                early_out[way, n, s] = raw(s, chips[1 + way] * per_y + 2 * owners[REACH.index(dz)] + 1 - way)
        copy = remote(early_out.at[way], early_in.at[way], raw_send.at[10 + way], raw_recv.at[10 + way], (next_y, prev_y)[way])
        copy.start()
        earlies.append(copy)

    mark("p06_wait_energy")
    others = energy.at[pl.ds(1, len(near))]
    cells = nx * ny * nz * nd_dev

    def told(src, dst, peer, recv):
        return remote(peaks.at[src], peaks.at[dst], small_send.at[1], small_recv.at[recv], peer)

    @pl.when(core == 1)
    def _():
        pltpu.make_async_copy(others, others, small_recv.at[0]).wait()
        for dy in range(ny_dev):
            both = jnp.sum(energy[dy * nd_dev : (dy + 1) * nd_dev], axis=0)
            mean = jnp.sum(both, axis=1, keepdims=True) / cells
            peaks[0, dy * shots : (dy + 1) * shots] = jnp.broadcast_to(mean, (shots, nz))
        for peers in (cross_core, along):
            for i, peer in enumerate(peers):
                told(0, nz_dev - 1 - i, peer, 1).start()
        told(0, 0, {"shot": shot, "depth": depth - 1}, 2).start()

    @pl.when(core == 0)
    def _():
        pltpu.make_async_copy(peaks.at[0], peaks.at[0], small_recv.at[2]).wait()

    for way in range(2):
        push(beside_out.at[way], beside_in.at[way], 4 + way, (next_z, prev_z)[way])
    rest = peaks.at[pl.ds(1, len(along))]
    mark("p08_wait_peak")
    pltpu.make_async_copy(rest, rest, small_recv.at[1]).wait()
    mark("p09_weights")
    peak = jnp.max(jnp.max(peaks[...], axis=0), axis=0, keepdims=True)
    scale = 1.0 / float(shots * ny_dev * nz_dev) ** 0.5
    weights = {dz: scale / jnp.sqrt(peaks[dz] + 0.5 * peak + 1.0) for dz in (0, 1, nz_dev - 1)}

    def weight(dy, dz, s):
        return jnp.broadcast_to(weights[dz][dy * shots + s : dy * shots + s + 1], (ny, nz))

    def blend(dy, dz, value):
        return sum(weight(dy, dz, s) * value(s) for s in range(shots))

    for g in range(groups):
        mixed[g] = blend(0, 0, lambda s: side_v[s, g])

    mark("p10_ysend")
    for copy in raws[:8]:
        copy.wait_recv()

    low, high = nz_dev - 1, 1
    behind, ahead = ny_dev - 1, 1

    def share(i, chip, j):
        x = chips[chip] * per_y + 2 * owners[i] + j
        total = blend(0, 0, lambda s: filt[s, x]) - ends_of(mixed[x // group], x)
        onward = chip and j == chip - 1
        side = (behind, ahead)[j]
        if onward:
            total = total + blend(side, 0, lambda s: raw_in[j, s, i])
        if not chip and REACH[i] in EARLY[1 - j]:
            n = EARLY[1 - j].index(REACH[i])
            total = total + blend((behind, ahead)[1 - j], 0, lambda s: early_in[1 - j, n, s])
        if REACH[i] == (3, -3)[j]:
            total = total + blend(0, (low, high)[j], lambda s: cross_in[j, s, chip])
            if onward:
                total = total + blend(side, (low, high)[j], lambda s: corner_in[3 * j, 1, s])
        if REACH[i] in (1, -1):
            way = (1, -1).index(REACH[i])
            if chip:
                total = total + blend(0, (low, high)[way], lambda s: beside_in[way, j, s, chip - 1])
            if onward:
                total = total + blend(side, (low, high)[way], lambda s: corner_in[2 * way + j, 0, s])
        return total

    def rows_of(way, i):
        return (way,) if REACH[i] in EARLY[way] else (0, 1)

    moves, finals = [], []
    for i in range(len(owners)):
        if i == 2:
            for way in range(2):
                for j in range(2):
                    x = y * per_y + 2 * seconds[way] + j
                    direct[way, j] = blend(0, 0, lambda s: filt[s, x]) - ends_of(mixed[x // group], x)
                slot = len(REACH) + way
                copy = remote(direct.at[way], arrived.at[slot], last_send.at[slot], last_recv.at[slot], along[(1, nz_dev - 3)[way]])
                copy.start()
                finals.append((copy, slot))
            for copy in raws[8:]:
                copy.wait_recv()
        for way, peer in enumerate((next_y, prev_y)):
            for j in rows_of(way, i):
                sent[way, i, j] = share(i, 1 + way, j)
            part = pl.ds(rows_of(way, i)[0], len(rows_of(way, i)))
            copy = remote(sent.at[way, i, part], got.at[way, i, part], move_send.at[way, i], move_recv.at[way, i], peer)
            moves.append(copy)
            copy.start()
    for copy in earlies:
        copy.wait_recv()
    for i in range(len(owners)):
        for j in range(2):
            image[i, j] = share(i, 0, j)

    mark("p10b_turn")

    mark("p11_zsend")
    for i, dz in enumerate(REACH):
        for way in range(2):
            moves[2 * i + way].wait_recv()
        for j in range(2):
            value = image[i, j]
            for way in range(2):
                if j in rows_of(way, i):
                    value = value + got[way, i, j]
            image[i, j] = value
        if dz:
            peer = along[(dz - 1) % nz_dev]
            copy = remote(image.at[i], arrived.at[i], last_send.at[i], last_recv.at[i], peer)
            copy.start()
            finals.append((copy, i))
    mark("p12_zwait")
    result = image[REACH.index(0)]
    for copy, slot in finals:
        copy.wait_recv()
        result = result + arrived[slot]
    out[...] = result

    mark("p13_tail")
    for copy, _ in finals:
        copy.wait_send()
    for copy in raws + earlies + moves:
        copy.wait_send()

    for k in range(2):
        part = energy.at[pl.ds(1, len(near) // 2 + 1 - k)]
        pl.when(core == k)(pltpu.make_async_copy(part, part, small_send.at[0]).wait)

    @pl.when(core == 1)
    def _():
        pltpu.make_async_copy(rest, rest, small_send.at[1]).wait()
        pltpu.make_async_copy(peaks, peaks, small_send.at[1]).wait()


    @pl.when(depth < nd_dev - 1)
    def _():
        up.wait_send()

    @pl.when(depth > 0)
    def _():
        down.wait_send()

    mark(None)


def solution(mesh):
    nd_dev = mesh.shape["depth"]
    ny_dev = ROWS_Y
    nz_dev = mesh.shape["shot"] // ny_dev

    def on_device(correlation, illumination, aperture):
        shots, nx, ny, nz = correlation.shape
        per_z = nx // ny_dev // nz_dev
        assert per_z == 2 and nz == 128 and nx == 64 and nz_dev == 8
        dma = pltpu.SemaphoreType.DMA
        field = (ny, nz)
        chunks = len(REACH)
        return pl.pallas_call(
            functools.partial(kernel, ny_dev, nz_dev, nd_dev),
            out_shape=jax.ShapeDtypeStruct((per_z, ny, nz), F32),
            in_specs=[pl.BlockSpec(memory_space=pl.ANY)] * 3,
            out_specs=pl.BlockSpec(memory_space=pltpu.VMEM),
            scratch_shapes=[
                pltpu.SMEM((shots, 4), jnp.int32),
                pltpu.VMEM((shots, nx, *field), F32),
                pltpu.VMEM((shots, nx, *field), F32),
                pltpu.VMEM((shots, nx + 2, ny + 2 * PAD, nz), F32),
                pltpu.VMEM((shots, nx, *field), F32),
                pltpu.VMEM((shots, *field), F32),
                pltpu.VMEM(field, F32),
                pltpu.VMEM(field, F32),
                pltpu.VMEM((shots, 2, *field), F32),
                pltpu.VMEM((shots, 2, *field), F32),
                pltpu.VMEM((shots, 2, *field), F32),
                pltpu.VMEM((2, *field), F32),
                pltpu.VMEM((ny_dev * nd_dev, shots, nz), F32),
                pltpu.VMEM((nz_dev, ny_dev * shots, nz), F32),
                pltpu.VMEM((2, shots, chunks, *field), F32),
                pltpu.VMEM((2, shots, chunks, *field), F32),
                pltpu.VMEM((2, shots, 3, *field), F32),
                pltpu.VMEM((2, shots, 3, *field), F32),
                pltpu.VMEM((2, 2, shots, 2, *field), F32),
                pltpu.VMEM((2, 2, shots, 2, *field), F32),
                pltpu.VMEM((4, 2, shots, *field), F32),
                pltpu.VMEM((4, 2, shots, *field), F32),
                pltpu.VMEM((2, 2, shots, *field), F32),
                pltpu.VMEM((2, 2, shots, *field), F32),
                pltpu.VMEM((2, per_z, *field), F32),
                pltpu.VMEM((2, chunks, per_z, *field), F32),
                pltpu.VMEM((2, chunks, per_z, *field), F32),
                pltpu.VMEM((chunks, per_z, *field), F32),
                pltpu.VMEM((chunks + 2, per_z, *field), F32),
                dma, dma((shots, PIECES, 2)),
                dma((2,)), dma((2,)), dma((2,)), dma((3,)),
                dma((12,)), dma((12,)), dma((2, chunks)), dma((2, chunks)),
                dma((chunks + 2,)), dma((chunks + 2,)),
            ],
            compiler_params=pltpu.CompilerParams(
                collective_id=0, has_side_effects=True, vmem_limit_bytes=32 << 20
            ),
        )(*(pltpu.with_memory_space_constraint(a, pltpu.HBM) for a in (aperture, correlation, illumination)))

    return jax.shard_map(
        on_device,
        mesh=mesh,
        in_specs=(P("shot", None, None, "depth"), P("shot", None, None, "depth"), P("shot", None)),
        out_specs=P("shot", None, "depth"),
        check_vma=False,
    )
```

```python
import functools

import jax
import jax.numpy as jnp
from jax import lax
from jax.experimental import pallas as pl
from jax.experimental.pallas import tpu as pltpu
from jax.sharding import PartitionSpec as P

ROWS_Y = 4
PIECES = 4
NORM_ROWS = 16
FILTER_ROWS = 16
PAD = 8
REACH = (3, -3, 1, 0, -1)
EARLY = ((0, 3), (0, -3))
F32 = jnp.float32
MESH = pl.DeviceIdType.MESH


class Marks:
    def __init__(self):
        self.scope = None

    def __call__(self, name):
        if self.scope is not None:
            self.scope.__exit__(None, None, None)
            self.scope = None
        if name:
            self.scope = jax.named_scope(name)
            self.scope.__enter__()


def kernel(
    ny_dev, nz_dev, nd_dev,
    box_hbm, corr, illum, out,
    box, corr_v, illum_v, norm, filt, edge, edge_low, edge_high, rim_v, wrap_v, side_v, mixed,
    energy, peaks, raw_out, raw_in, cross_out, cross_in, beside_out, beside_in, corner_out, corner_in, early_out, early_in, direct, sent, got, image, arrived,
    box_sem, load_sem, edge_send, edge_recv, small_send, small_recv,
    raw_send, raw_recv, move_send, move_recv, last_send, last_recv,
):
    shots, nx, ny, nz = filt.shape
    mark = Marks()
    mark("p00_load_signal")
    shot, depth = lax.axis_index("shot"), lax.axis_index("depth")
    y, z = shot // nz_dev, shot % nz_dev
    per_y = nx // ny_dev
    group = nz // 4
    groups = nx // group

    box_load = pltpu.make_async_copy(box_hbm, box, box_sem)
    box_load.start()
    step = nx // PIECES
    loads = []
    for c in range(PIECES):
        piece = []
        for s in range(shots):
            rows = pl.ds(c * step, step)
            piece.append(pltpu.make_async_copy(corr.at[s, rows], corr_v.at[s, rows], load_sem.at[s, c, 0]))
            piece.append(pltpu.make_async_copy(illum.at[s, rows], illum_v.at[s, rows], load_sem.at[s, c, 1]))
        loads.append(piece)
    for copy in loads[0]:
        copy.start()

    near = []
    for dy in range(ny_dev):
        for dd in range(nd_dev):
            if dy or dd:
                near.append({
                    "shot": lax.rem(y + dy, ny_dev) * nz_dev + z,
                    "depth": lax.rem(depth + dd, nd_dev),
                })
    along = [
        {"shot": y * nz_dev + lax.rem(z + dz, nz_dev), "depth": depth} for dz in range(1, nz_dev)
    ]
    after, before, across = (lax.rem(y + d, ny_dev) for d in (1, ny_dev - 1, ny_dev // 2))
    corners = [
        {"shot": side * nz_dev + lax.rem(z + d, nz_dev), "depth": depth}
        for d in (1, nz_dev - 1)
        for side in (after, before)
    ]
    barrier = pltpu.get_barrier_semaphore()
    core = lax.rem(depth, 2)
    cross_core = [{"shot": peer["shot"], "depth": depth + 1 - 2 * core} for peer in along]

    def hops(count, d):
        return min(d, count - d)

    far = [hops(ny_dev, (i + 1) // nd_dev) + hops(nd_dev, (i + 1) % nd_dev) / 2 for i in range(len(near))]
    far += [hops(nz_dev, i + 1) for i in range(len(along))] * 2 + [2] * len(corners)
    greeted = near + along + cross_core + corners
    for i in sorted(range(len(greeted)), key=lambda i: -far[i]):
        peer = greeted[i]
        pl.semaphore_signal(barrier, inc=1, device_id=peer, device_id_type=MESH)
    for piece in loads[1:]:
        for copy in piece:
            copy.start()

    lane = lax.broadcasted_iota(jnp.int32, (ny, nz), 1)
    row = lax.broadcasted_iota(jnp.int32, (ny, nz), 0)
    ends = (lane == 0) | (lane == nz - 1)
    top, bottom = row == 0, row == ny - 1
    column = lane // 4
    place = lax.rem(lane, 4)
    zero = jnp.zeros((ny, nz), F32)

    def beside_rows(here):
        return jnp.where(top, 0.0, pltpu.roll(here, 1, 0)) + jnp.where(bottom, 0.0, pltpu.roll(here, ny - 1, 0))

    strips = [((row >= box[s, 2]) & (row < box[s, 3])).astype(F32) for s in range(shots)]
    bounds = [(box[s, 0], box[s, 1]) for s in range(shots)]
    blank = jnp.zeros((PAD, nz), F32)

    def clear(x, carry):
        for s in range(shots):
            norm[s, x, :PAD] = blank
            norm[s, x, PAD + ny :] = blank
        return carry

    lax.fori_loop(1, nx + 1, clear, 0)
    for s in range(shots):
        for x in (0, nx + 1):
            norm[s, x] = jnp.zeros((ny + 2 * PAD, nz), F32)
    box_load.wait()
    strips = [((row >= box[s, 2]) & (row < box[s, 3])).astype(F32) for s in range(shots)]
    bounds = [(box[s, 0], box[s, 1]) for s in range(shots)]

    def normalize(k, packs):
        packs = list(packs)
        for s in range(shots):
            for j in range(NORM_ROWS):
                x = k * NORM_ROWS + j
                inside = jnp.where((x >= bounds[s][0]) & (x < bounds[s][1]), 1.0, 0.0).astype(F32)
                value = (strips[s] * inside) * corr_v[s, x] / (illum_v[s, x] + 0.1)
                norm[s, x + 1, PAD : PAD + ny] = value
                turned = pltpu.roll(value, lax.rem(4 * x + 2, nz), 1)
                packs[s] = jnp.where(column == lax.rem(x, group), turned, packs[s])
        return tuple(packs)

    def filter_block(k, sums):
        sums = list(sums)
        for s in range(shots):
            base = k * FILTER_ROWS
            rows = [norm[s, base + i, PAD : PAD + ny] for i in range(FILTER_ROWS + 2)]
            for j in range(FILTER_ROWS):
                here = rows[j + 1]
                beside = rows[j] + rows[j + 2] + (norm[s, base + j + 1, pl.ds(PAD - 1 + lax.min(k, 0), ny)] + norm[s, base + j + 1, pl.ds(PAD + 1 + lax.min(k, 0), ny)])
                beside = beside + pltpu.roll(here, 1, 1) + pltpu.roll(here, nz - 1, 1)
                value = 6.0 * here - beside
                filt[s, base + j] = value
                sums[s] = sums[s] + value * value
        return tuple(sums)

    packs, packed = (zero,) * shots, []
    for c in range(PIECES):
        mark(f"p01_w{c}")
        for copy in loads[c]:
            copy.wait()
        mark(f"p01_x{c}")
        blocks = step // NORM_ROWS
        packs = lax.fori_loop(c * blocks, (c + 1) * blocks, normalize, packs)
        if (c + 1) * step % group == 0:
            packed.append(packs)
            packs = (zero,) * shots

    mark("p02_pack")
    inner = (place == 1) | (place == 2)
    rims = [jnp.where(inner, packed[0][s], pltpu.roll(packed[1][s], 2, 1)) for s in range(shots)]
    odd = lax.rem(lane, 2) == 1
    edge[0] = jnp.where(odd, rims[0], pltpu.roll(rims[1], 1, 1))
    edge[1] = jnp.where(odd, pltpu.roll(rims[1], nz - 1, 1), rims[0])

    mark("p02b_barrier")
    pl.semaphore_wait(barrier, len(near) + len(along) + len(cross_core) + len(corners))
    mark("p03_halo")

    def remote(src, dst, send, recv, peer):
        return pltpu.make_async_remote_copy(
            src_ref=src, dst_ref=dst, send_sem=send, recv_sem=recv, device_id=peer, device_id_type=MESH
        )

    up = remote(edge.at[0], edge_low, edge_send.at[0], edge_recv.at[0], {"shot": shot, "depth": lax.rem(depth + 1, nd_dev)})
    down = remote(edge.at[1], edge_high, edge_send.at[1], edge_recv.at[1], {"shot": shot, "depth": lax.rem(depth + nd_dev - 1, nd_dev)})

    @pl.when(depth < nd_dev - 1)
    def _():
        up.start()

    @pl.when(depth > 0)
    def _():
        down.start()

    @pl.when(depth == 0)
    def _():
        edge_low[...] = jnp.zeros_like(edge_low)

    @pl.when(depth == nd_dev - 1)
    def _():
        edge_high[...] = jnp.zeros_like(edge_high)

    mark("p03_filter")
    sums = lax.fori_loop(0, nx // FILTER_ROWS, filter_block, (zero,) * shots)

    mark("p03a_rim")
    for s in range(shots):
        parts = [packed[g][s] for g in range(groups)]
        backs = [pltpu.roll(part, 4, 1) for part in parts]
        aheads = [pltpu.roll(part, nz - 4, 1) for part in parts]
        for g, part in enumerate(parts):
            back = jnp.where(lane < 4, backs[g - 1] if g else 0.0, backs[g])
            ahead = jnp.where(lane >= nz - 4, aheads[g + 1] if g < groups - 1 else 0.0, aheads[g])
            lower, higher = pltpu.roll(part, 1, 1), pltpu.roll(part, nz - 1, 1)
            deep = jnp.where(place == 1, lower, higher)
            rim_v[s, g] = 6.0 * part - (back + ahead + beside_rows(part) + deep)
            wrap_v[s, g] = jnp.where(place == 1, higher, lower)

    mark("p03w_halo")
    @pl.when(depth > 0)
    def _():
        up.wait_recv()

    @pl.when(depth < nd_dev - 1)
    def _():
        down.wait_recv()

    mark("p04_energy")
    for s in range(shots):
        total = jnp.where(ends, 0.0, sums[s])
        high, low = edge_high[...], edge_low[...]
        for g in range(groups):
            side = jnp.where(
                place == 1,
                pltpu.roll(high, (nz - 1 - 2 * g + s) % nz, 1),
                pltpu.roll(low, (nz + 1 - 2 * g - s) % nz, 1),
            )
            side_v[s, g] = side - wrap_v[s, g]
            rim = rim_v[s, g] - side
            total = total + jnp.where(inner, rim * rim, 0.0)
        energy[0, s : s + 1] = jnp.sum(total, axis=0, keepdims=True)

    def span(i):
        dy, dd = (i + 1) // nd_dev, (i + 1) % nd_dev
        return min(dy, ny_dev - dy) + min(dd, nd_dev - dd) / 2

    for i in sorted(range(len(near)), key=span, reverse=True):
        dy, dd = (i + 1) // nd_dev, (i + 1) % nd_dev
        peer = near[i]
        slot = ((ny_dev - dy) % ny_dev) * nd_dev + (nd_dev - dd) % nd_dev
        copy = remote(energy.at[0], energy.at[slot], small_send.at[0], small_recv.at[0], peer)
        pl.when(core == 1 - dd % 2)(copy.start)

    mark("p05_raw")
    next_y = {"shot": after * nz_dev + z, "depth": depth}
    prev_y = {"shot": before * nz_dev + z, "depth": depth}
    next_z, prev_z = along[0], along[-1]
    owners = [lax.rem(z + nz_dev + dz, nz_dev) for dz in REACH]
    opposite = lax.rem(z + nz_dev // 2, nz_dev)
    seconds = [lax.rem(z + 2, nz_dev), lax.rem(z + nz_dev - 2, nz_dev)]

    def ends_of(packed_side, x):
        return jnp.where(ends, pltpu.roll(packed_side, lax.rem(2 * nz - 2 - 4 * lax.rem(x, group), nz), 1), 0.0)

    def raw(s, x):
        return filt[s, x] - ends_of(side_v[s, x // group], x)

    chips = (y, after, before)
    raws = []

    def push(out_ref, in_ref, index, peer):
        copy = remote(out_ref, in_ref, raw_send.at[index], raw_recv.at[index], peer)
        copy.start()
        raws.append(copy)

    for way in range(2):
        for s in range(shots):
            for i, chip in enumerate(chips):
                cross_out[way, s, i] = raw(s, chip * per_y + 2 * opposite + way)
    for way in range(2):
        push(cross_out.at[way], cross_in.at[way], way, (next_z, prev_z)[way])
    for way in range(2):
        for s in range(shots):
            for i, owner in enumerate(owners):
                raw_out[way, s, i] = raw(s, across * per_y + 2 * owner + way)
    for way in range(2):
        push(raw_out.at[way], raw_in.at[way], 2 + way, (next_y, prev_y)[way])
    for way in range(2):
        for j in range(2):
            for s in range(shots):
                for i, chip in enumerate(chips[1:]):
                    beside_out[way, j, s, i] = raw(s, chip * per_y + 2 * seconds[way] + j)
    for way in range(2):
        for j in range(2):
            for s in range(shots):
                corner_out[2 * way + j, 0, s] = raw(s, across * per_y + 2 * seconds[way] + j)
                if j == way:
                    corner_out[2 * way + j, 1, s] = raw(s, across * per_y + 2 * opposite + j)
    for k in range(4):
        part = pl.ds(0, 2 if k in (0, 3) else 1)
        push(corner_out.at[k, part], corner_in.at[k, part], 6 + k, corners[k])
    earlies = []
    for way in range(2):
        for n, dz in enumerate(EARLY[way]):
            for s in range(shots):
                early_out[way, n, s] = raw(s, chips[1 + way] * per_y + 2 * owners[REACH.index(dz)] + 1 - way)
        copy = remote(early_out.at[way], early_in.at[way], raw_send.at[10 + way], raw_recv.at[10 + way], (next_y, prev_y)[way])
        copy.start()
        earlies.append(copy)

    mark("p06_wait_energy")
    others = energy.at[pl.ds(1, len(near))]
    cells = nx * ny * nz * nd_dev

    def told(src, dst, peer, recv):
        return remote(peaks.at[src], peaks.at[dst], small_send.at[1], small_recv.at[recv], peer)

    @pl.when(core == 1)
    def _():
        pltpu.make_async_copy(others, others, small_recv.at[0]).wait()
        for dy in range(ny_dev):
            both = jnp.sum(energy[dy * nd_dev : (dy + 1) * nd_dev], axis=0)
            mean = jnp.sum(both, axis=1, keepdims=True) / cells
            peaks[0, dy * shots : (dy + 1) * shots] = jnp.broadcast_to(mean, (shots, nz))
        for peers in (cross_core, along):
            for i, peer in enumerate(peers):
                told(0, nz_dev - 1 - i, peer, 1).start()
        told(0, 0, {"shot": shot, "depth": depth - 1}, 2).start()

    @pl.when(core == 0)
    def _():
        pltpu.make_async_copy(peaks.at[0], peaks.at[0], small_recv.at[2]).wait()

    for way in range(2):
        push(beside_out.at[way], beside_in.at[way], 4 + way, (next_z, prev_z)[way])
    rest = peaks.at[pl.ds(1, len(along))]
    mark("p08_wait_peak")
    pltpu.make_async_copy(rest, rest, small_recv.at[1]).wait()
    mark("p09_weights")
    peak = jnp.max(jnp.max(peaks[...], axis=0), axis=0, keepdims=True)
    scale = 1.0 / float(shots * ny_dev * nz_dev) ** 0.5
    weights = {dz: scale / jnp.sqrt(peaks[dz] + 0.5 * peak + 1.0) for dz in (0, 1, nz_dev - 1)}

    def weight(dy, dz, s):
        return jnp.broadcast_to(weights[dz][dy * shots + s : dy * shots + s + 1], (ny, nz))

    def blend(dy, dz, value):
        return sum(weight(dy, dz, s) * value(s) for s in range(shots))

    for g in range(groups):
        mixed[g] = blend(0, 0, lambda s: side_v[s, g])

    mark("p10_ysend")
    for copy in raws[:8]:
        copy.wait_recv()

    low, high = nz_dev - 1, 1
    behind, ahead = ny_dev - 1, 1

    def share(i, chip, j):
        x = chips[chip] * per_y + 2 * owners[i] + j
        total = blend(0, 0, lambda s: filt[s, x]) - ends_of(mixed[x // group], x)
        onward = chip and j == chip - 1
        side = (behind, ahead)[j]
        if onward:
            total = total + blend(side, 0, lambda s: raw_in[j, s, i])
        if not chip and REACH[i] in EARLY[1 - j]:
            n = EARLY[1 - j].index(REACH[i])
            total = total + blend((behind, ahead)[1 - j], 0, lambda s: early_in[1 - j, n, s])
        if REACH[i] == (3, -3)[j]:
            total = total + blend(0, (low, high)[j], lambda s: cross_in[j, s, chip])
            if onward:
                total = total + blend(side, (low, high)[j], lambda s: corner_in[3 * j, 1, s])
        if REACH[i] in (1, -1):
            way = (1, -1).index(REACH[i])
            if chip:
                total = total + blend(0, (low, high)[way], lambda s: beside_in[way, j, s, chip - 1])
            if onward:
                total = total + blend(side, (low, high)[way], lambda s: corner_in[2 * way + j, 0, s])
        return total

    def rows_of(way, i):
        return (way,) if REACH[i] in EARLY[way] else (0, 1)

    moves, finals = [], []
    for i in range(len(owners)):
        if i == 2:
            for way in range(2):
                for j in range(2):
                    x = y * per_y + 2 * seconds[way] + j
                    direct[way, j] = blend(0, 0, lambda s: filt[s, x]) - ends_of(mixed[x // group], x)
                slot = len(REACH) + way
                copy = remote(direct.at[way], arrived.at[slot], last_send.at[slot], last_recv.at[slot], along[(1, nz_dev - 3)[way]])
                copy.start()
                finals.append((copy, slot))
            for copy in raws[8:]:
                copy.wait_recv()
        for way, peer in enumerate((next_y, prev_y)):
            for j in rows_of(way, i):
                sent[way, i, j] = share(i, 1 + way, j)
            part = pl.ds(rows_of(way, i)[0], len(rows_of(way, i)))
            copy = remote(sent.at[way, i, part], got.at[way, i, part], move_send.at[way, i], move_recv.at[way, i], peer)
            moves.append(copy)
            copy.start()
    for copy in earlies:
        copy.wait_recv()
    for i in range(len(owners)):
        for j in range(2):
            image[i, j] = share(i, 0, j)

    mark("p10b_turn")

    mark("p11_zsend")
    for i, dz in enumerate(REACH):
        for way in range(2):
            moves[2 * i + way].wait_recv()
        for j in range(2):
            value = image[i, j]
            for way in range(2):
                if j in rows_of(way, i):
                    value = value + got[way, i, j]
            image[i, j] = value
        if dz:
            peer = along[(dz - 1) % nz_dev]
            copy = remote(image.at[i], arrived.at[i], last_send.at[i], last_recv.at[i], peer)
            copy.start()
            finals.append((copy, i))
    mark("p12_zwait")
    result = image[REACH.index(0)]
    for copy, slot in finals:
        copy.wait_recv()
        result = result + arrived[slot]
    out[...] = result

    mark("p13_tail")
    for copy, _ in finals:
        copy.wait_send()
    for copy in raws + earlies + moves:
        copy.wait_send()

    for k in range(2):
        part = energy.at[pl.ds(1, len(near) // 2 + 1 - k)]
        pl.when(core == k)(pltpu.make_async_copy(part, part, small_send.at[0]).wait)

    @pl.when(core == 1)
    def _():
        pltpu.make_async_copy(rest, rest, small_send.at[1]).wait()
        pltpu.make_async_copy(peaks, peaks, small_send.at[1]).wait()


    @pl.when(depth < nd_dev - 1)
    def _():
        up.wait_send()

    @pl.when(depth > 0)
    def _():
        down.wait_send()

    mark(None)


def solution(mesh):
    nd_dev = mesh.shape["depth"]
    ny_dev = ROWS_Y
    nz_dev = mesh.shape["shot"] // ny_dev

    def on_device(correlation, illumination, aperture):
        shots, nx, ny, nz = correlation.shape
        per_z = nx // ny_dev // nz_dev
        assert per_z == 2 and nz == 128 and nx == 64 and nz_dev == 8
        dma = pltpu.SemaphoreType.DMA
        field = (ny, nz)
        chunks = len(REACH)
        return pl.pallas_call(
            functools.partial(kernel, ny_dev, nz_dev, nd_dev),
            out_shape=jax.ShapeDtypeStruct((per_z, ny, nz), F32),
            in_specs=[pl.BlockSpec(memory_space=pl.ANY)] * 3,
            out_specs=pl.BlockSpec(memory_space=pltpu.VMEM),
            scratch_shapes=[
                pltpu.SMEM((shots, 4), jnp.int32),
                pltpu.VMEM((shots, nx, *field), F32),
                pltpu.VMEM((shots, nx, *field), F32),
                pltpu.VMEM((shots, nx + 2, ny + 2 * PAD, nz), F32),
                pltpu.VMEM((shots, nx, *field), F32),
                pltpu.VMEM((shots, *field), F32),
                pltpu.VMEM(field, F32),
                pltpu.VMEM(field, F32),
                pltpu.VMEM((shots, 2, *field), F32),
                pltpu.VMEM((shots, 2, *field), F32),
                pltpu.VMEM((shots, 2, *field), F32),
                pltpu.VMEM((2, *field), F32),
                pltpu.VMEM((ny_dev * nd_dev, shots, nz), F32),
                pltpu.VMEM((nz_dev, ny_dev * shots, nz), F32),
                pltpu.VMEM((2, shots, chunks, *field), F32),
                pltpu.VMEM((2, shots, chunks, *field), F32),
                pltpu.VMEM((2, shots, 3, *field), F32),
                pltpu.VMEM((2, shots, 3, *field), F32),
                pltpu.VMEM((2, 2, shots, 2, *field), F32),
                pltpu.VMEM((2, 2, shots, 2, *field), F32),
                pltpu.VMEM((4, 2, shots, *field), F32),
                pltpu.VMEM((4, 2, shots, *field), F32),
                pltpu.VMEM((2, 2, shots, *field), F32),
                pltpu.VMEM((2, 2, shots, *field), F32),
                pltpu.VMEM((2, per_z, *field), F32),
                pltpu.VMEM((2, chunks, per_z, *field), F32),
                pltpu.VMEM((2, chunks, per_z, *field), F32),
                pltpu.VMEM((chunks, per_z, *field), F32),
                pltpu.VMEM((chunks + 2, per_z, *field), F32),
                dma, dma((shots, PIECES, 2)),
                dma((2,)), dma((2,)), dma((2,)), dma((3,)),
                dma((12,)), dma((12,)), dma((2, chunks)), dma((2, chunks)),
                dma((chunks + 2,)), dma((chunks + 2,)),
            ],
            compiler_params=pltpu.CompilerParams(
                collective_id=0, has_side_effects=True, vmem_limit_bytes=32 << 20
            ),
        )(*(pltpu.with_memory_space_constraint(a, pltpu.HBM) for a in (aperture, correlation, illumination)))

    return jax.shard_map(
        on_device,
        mesh=mesh,
        in_specs=(P("shot", None, None, "depth"), P("shot", None, None, "depth"), P("shot", None)),
        out_specs=P("shot", None, "depth"),
        check_vma=False,
    )
```
